32 devices in a mesh: rep: 2 (over y), seq: 4 (over z), head: 4 (over x, core).
Axes of the slice: x: 2, y: 2, z: 4, core: 2. Of those that a mesh axis runs over, the one named last changes fastest.
Arguments:
- queries: bfloat16 [2048, 4096], P(('rep', 'seq'), 'head'), parts along dimension 0, may hold values from -520 to 520
- rotated_key_states: bfloat16 [2048, 1024], P(('rep', 'seq'), 'head'), parts along dimension 0, may hold values from -6 to 6
- value_state_array: bfloat16 [2048, 1024], P(('rep', 'seq'), 'head'), parts along dimension 0, may hold values from -6 to 6
- residual: bfloat16 [2048, 4096], P(('rep', 'seq'), 'head'), parts along dimension 0, may hold values from -60 to 60
- out_weight: bfloat16 [4096, 4096], P('head'), may hold values from -0.75 to 0.75
- norm_gain: bfloat16 [4096], P('head'), may hold values from 0.5 to 1.5
- block_order: int32 [16], P('rep'), parts along dimension 0, may hold values from 0 to 7, as said below
Outputs:
- normed: bfloat16 [2048, 4096], P(('rep', 'seq'), 'head'), parts along dimension 0
The draws below stay inside these ranges and needn't reach their ends.
There are 2 independent parts, one for each index of `rep`. The reference program is written for one: setup_inputs(seed, part) draws one part's arguments, and reference() takes and returns one part's arrays. A program takes and returns all parts, laid end to end along the dimension named above; an argument that names none is the same for every part. Nothing has to cross between parts.
Inputs may be any that keep to these rules, and one draw needn't show every extreme that they name: `block_order`: slots 2i and 2i + 1 hold blocks c and 7 - c in either order; every block appears once.
All inputs are finite; a program needn't handle non-finite values.
Results may differ from the reference program's by a relative error of at most 0.008.
Values may be sent and summed in bfloat16 or wider, within the bound.
A program may use at most 64 MiB of HBM per device.

```python
import math
import jax
import jax.numpy as jnp
from jax import lax

D = 4096
QUERY_HEADS = 32
KEY_VALUE_HEADS = 8
HEAD_SIZE = 128
SEQUENCE_BLOCK = 128
BLOCKS = 8
SEQUENCE_LENGTH = 1024


def paired_heads(key):
    base_key = jax.random.fold_in(key, 7)
    query_key, random_key_for_keys = jax.random.split(base_key, 2)
    unrotated_queries = jnp.clip(jax.random.normal(query_key, (SEQUENCE_LENGTH, QUERY_HEADS * HEAD_SIZE), jnp.float32) * 1.5, -9.0, 9.0)
    unrotated_keys = jnp.clip(jax.random.normal(random_key_for_keys, (SEQUENCE_LENGTH, KEY_VALUE_HEADS, HEAD_SIZE), jnp.float32), -6.0, 6.0)
    return (unrotated_queries, unrotated_keys.reshape(SEQUENCE_LENGTH, KEY_VALUE_HEADS * HEAD_SIZE))


def draw_queries(key, part):
    return paired_heads(key)[0].astype(jnp.bfloat16)


def draw_rotated_key_states(key, part):
    return paired_heads(key)[1].astype(jnp.bfloat16)


def draw_residual(key, part):
    row_key, column_key, entry_key = jax.random.split(jax.random.fold_in(key, 5), 3)
    row_scale = jnp.exp(jax.random.uniform(row_key, (SEQUENCE_LENGTH, 1), jnp.float32, math.log(0.3), math.log(3.0)))
    column_place = jnp.arange(D, dtype=jnp.float32) / D
    jitter = jax.random.uniform(column_key, (D,), jnp.float32, 0.7, 1.3)
    column_scale = jnp.power(3.0, column_place) * jitter
    entries = jnp.clip(jax.random.normal(entry_key, (SEQUENCE_LENGTH, D), jnp.float32), -5.0, 5.0)
    return (entries * row_scale * column_scale[None, :]).astype(jnp.bfloat16)


def draw_block_order(key, part):
    pair_key, flip_key = jax.random.split(jax.random.fold_in(key, 3))
    pair_count = BLOCKS // 2
    early_ids = jax.random.permutation(pair_key, pair_count).astype(jnp.int32)
    flip_bits = jax.random.randint(flip_key, (pair_count,), 0, 2)
    first_slot = jnp.where(flip_bits == 1, early_ids, BLOCKS - 1 - early_ids)
    second_slot = BLOCKS - 1 - first_slot
    return jnp.stack([first_slot, second_slot], axis=1).reshape(BLOCKS).astype(jnp.int32)


def level_of(own_key, shape, cuts, least, largest):
    factor_of, own = 1.0, jax.random.fold_in(own_key, 6)
    for dim, blocks in cuts:
        heights = jnp.exp(jax.random.uniform(jax.random.fold_in(own, dim), (blocks,), jnp.float32, least / len(cuts), largest / len(cuts)))
        factor_of = factor_of * jnp.repeat(heights, shape[dim] // blocks).reshape([-1 if axis == dim else 1 for axis in range(len(shape))])
    return factor_of


def centred(key, dims, deviation, reach, shards=(), kind=jnp.bfloat16):
    drawn = deviation * jax.random.normal(key, dims, jnp.float32)
    if shards:
        drawn = drawn * level_of(key, dims, shards, -0.22, 0.18)
    return jnp.clip(drawn, -reach, reach).astype(kind)


def setup_inputs(seed: int = 0, part: int = 0) -> dict:
    key_list = jax.random.split(jax.random.key(seed), 8)
    part_splits = jax.random.split(jax.random.fold_in(key_list[7], part), 8)
    return {
        "queries": draw_queries(jax.random.fold_in(jax.random.fold_in(key_list[7], part), 71), part),
        "rotated_key_states": draw_rotated_key_states(jax.random.fold_in(jax.random.fold_in(key_list[7], part), 71), part),
        "value_state_array": centred(part_splits[2], (SEQUENCE_LENGTH, KEY_VALUE_HEADS * HEAD_SIZE), 1.0, 6.0, ((0, 4), (1, 4))),
        "residual": draw_residual(jax.random.fold_in(jax.random.fold_in(key_list[7], part), 71), part),
        "out_weight": centred(key_list[4], (QUERY_HEADS * HEAD_SIZE, D), (HEAD_SIZE // 2) ** -0.5, 0.75, ((0, 4),)),
        "norm_gain": jnp.clip(1.0 + 0.1 * jax.random.normal(key_list[5], (D,), jnp.float32), 0.5, 1.5).astype(jnp.bfloat16),
        "block_order": draw_block_order(jax.random.fold_in(jax.random.fold_in(key_list[7], part), 71), part),
    }


norm_epsilon = 1e-05

def reference(queries, rotated_key_states, value_state_array, residual, out_weight, norm_gain, block_order):
    row_total_count = queries.shape[0]
    row_ids = jnp.arange(row_total_count, dtype=jnp.int32)
    positions = (block_order[row_ids // SEQUENCE_BLOCK] * SEQUENCE_BLOCK + row_ids % SEQUENCE_BLOCK).astype(jnp.int32)
    queries_per_group = QUERY_HEADS // KEY_VALUE_HEADS
    heads_of_keys = rotated_key_states.astype(jnp.float32).reshape(row_total_count, KEY_VALUE_HEADS, HEAD_SIZE)
    heads_of_values = value_state_array.astype(jnp.float32).reshape(row_total_count, KEY_VALUE_HEADS, HEAD_SIZE)
    heads_of_queries = queries.astype(jnp.float32).reshape(row_total_count // SEQUENCE_BLOCK, SEQUENCE_BLOCK, KEY_VALUE_HEADS, queries_per_group, HEAD_SIZE)
    query_positions = positions.reshape(row_total_count // SEQUENCE_BLOCK, SEQUENCE_BLOCK)

    def one_block(packed):
        block_queries, block_positions = packed
        scores = jnp.einsum('qhgd,khd->hgqk', block_queries, heads_of_keys, precision=lax.Precision.HIGHEST) * HEAD_SIZE ** (-0.5)
        visible = (positions[None, :] <= block_positions[:, None])[None, None]
        limited = jnp.where(visible, scores, -1e+30)
        row_peak = lax.optimization_barrier(jnp.max(limited, axis=3, keepdims=True))
        weights = jnp.where(visible, jnp.exp(limited - row_peak), 0.0)
        denominators = lax.optimization_barrier(jnp.sum(weights, axis=3))
        rounded = lax.optimization_barrier(weights.astype(jnp.bfloat16)).astype(jnp.float32)
        weighted_sum = jnp.einsum('hgqk,khd->hgqd', rounded, heads_of_values, precision=lax.Precision.HIGHEST)
        result = weighted_sum / denominators[..., None]
        return result.transpose(2, 0, 1, 3).reshape(SEQUENCE_BLOCK, QUERY_HEADS * HEAD_SIZE).astype(jnp.bfloat16)
    attention = lax.map(one_block, (heads_of_queries, query_positions)).reshape(row_total_count, QUERY_HEADS * HEAD_SIZE)
    mixed_rows = residual.astype(jnp.float32) + jnp.dot(attention, out_weight, preferred_element_type=jnp.float32)
    mean_square = lax.optimization_barrier(jnp.mean(mixed_rows * mixed_rows, axis=1))
    inverse = lax.rsqrt(mean_square + norm_epsilon)
    return (mixed_rows * inverse[:, None] * norm_gain.astype(jnp.float32)[None, :]).astype(jnp.bfloat16)
```

```python
import functools
import math

import jax
import jax.numpy as jnp
from jax import lax
from jax.experimental import pallas as pl
from jax.experimental.pallas import tpu as pltpu
from jax.sharding import PartitionSpec as P

MESH = pl.DeviceIdType.MESH
HEAD_SIZE = 128
NORM_EPSILON = 1e-05
MASKED = -1e30


def kernel(
    ns, nh, order_ref, k_hbm, v_hbm, gain_hbm, q_hbm, res_hbm, w_hbm, out_ref,
    k_ref, v_ref, gain_ref, q_vm, res_vm, q_stack, w_own, w_peer, kv, att, peer_att, part, part_in,
    ssq, ssq_in, acc, peak, denom, mixed, ahead,
    load_sem, local_sem, kv_send, kv_recv, w_send, w_recv, att_send, att_recv,
    part_send, part_recv, ssq_send, ssq_recv,
):
    seq, head = lax.axis_index("seq"), lax.axis_index("head")
    rows, width = q_vm.shape
    block = rows // 2
    kv_heads = k_ref.shape[1] // HEAD_SIZE
    group = width // k_ref.shape[1]
    features = res_vm.shape[1]
    pairs = nh // 2
    bit, pair = lax.rem(head, 2), head // 2
    sibling = head + 1 - 2 * bit
    keys = ns * block

    barrier = pltpu.get_barrier_semaphore()

    @pl.when(seq > 0)
    def _():
        pl.semaphore_signal(barrier, inc=1, device_id={"seq": seq - 1}, device_id_type=MESH)

    @pl.when(seq < ns - 1)
    def _():
        pl.semaphore_signal(barrier, inc=1, device_id={"seq": seq + 1}, device_id_type=MESH)

    for step in range(1, nh):
        pl.semaphore_signal(
            barrier, inc=1, device_id={"head": lax.rem(head + step, nh)}, device_id_type=MESH
        )
    q_copy = pltpu.make_async_copy(q_hbm, q_vm, local_sem.at[0])
    res_copy = pltpu.make_async_copy(res_hbm, res_vm, local_sem.at[1])
    loads = [
        pltpu.make_async_copy(source, target, load_sem.at[i])
        for i, (source, target) in enumerate(((k_hbm, k_ref), (v_hbm, v_ref), (gain_hbm, gain_ref)))
    ]
    for load in loads:
        load.start()
    q_copy.start()

    first, second = order_ref[2 * seq], order_ref[2 * seq + 1]
    early_id, late_id = jnp.minimum(first, second), jnp.maximum(first, second)
    swapped = jnp.where(first > second, 1, 0)

    def halves(ref):
        low, high = ref[:block, :].astype(jnp.float32), ref[block:, :].astype(jnp.float32)
        swap = jnp.full(low.shape, swapped, jnp.int32) != 0
        return jnp.where(swap, high, low), jnp.where(swap, low, high)

    for index, ref in ((0, k_ref), (1, v_ref)):
        loads[index].wait()
        early, late = halves(ref)
        kv[index, seq] = early.astype(jnp.bfloat16)
        kv[2 + index, seq] = late.astype(jnp.bfloat16)

    near = jnp.where(seq > 0, 1, 0) + jnp.where(seq < ns - 1, 1, 0)
    pl.semaphore_wait(barrier, near + nh - 1)

    def kv_copy(direction, chunk, distance):
        piece = seq - distance if direction == 0 else seq + distance
        target = seq + 1 if direction == 0 else seq - 1
        return pltpu.make_async_remote_copy(
            src_ref=kv.at[chunk, piece],
            dst_ref=kv.at[chunk, piece],
            send_sem=kv_send.at[direction, chunk, distance],
            recv_sem=kv_recv.at[chunk, piece],
            device_id={"seq": target},
            device_id_type=MESH,
        )

    def sends(direction, distance):
        if direction == 0:
            return jnp.logical_and(seq >= distance, seq < ns - 1)
        return jnp.logical_and(seq + distance <= ns - 1, seq > 0)

    def arrives(direction, distance):
        return seq >= distance if direction == 0 else seq + distance <= ns - 1

    def start_kv(chunk, distance):
        for direction in range(2):
            @pl.when(sends(direction, distance))
            def _():
                kv_copy(direction, chunk, distance).start()

    def forward_kv(chunk, distance):
        for direction in range(2):
            @pl.when(sends(direction, distance))
            def _():
                kv_copy(direction, chunk, distance).wait_recv()
                kv_copy(direction, chunk, distance).start()

    def collect_kv(chunks, distances):
        for distance in distances:
            for chunk in chunks:
                for direction in range(2):
                    @pl.when(
                        jnp.logical_and(
                            arrives(direction, distance),
                            jnp.logical_not(sends(direction, distance)),
                        )
                    )
                    def _():
                        kv_copy(direction, chunk, distance).wait_recv()

    for chunk in (0, 1, 2):
        start_kv(chunk, 0)

    def w_copies(index):
        mine = pl.ds(pl.multiple_of((2 * index + bit) * features, 128), features)
        theirs = pl.ds(pl.multiple_of((2 * index + 1 - bit) * features, 128), features)
        local = pltpu.make_async_copy(w_hbm.at[:, mine], w_own.at[index], local_sem.at[2 + index])
        remote = pltpu.make_async_remote_copy(
            src_ref=w_hbm.at[:, theirs],
            dst_ref=w_peer.at[index],
            send_sem=w_send.at[index],
            recv_sem=w_recv.at[index],
            device_id={"head": sibling},
            device_id_type=MESH,
        )
        return local, remote

    for index in range(pairs):
        local, remote = w_copies(index)
        remote.start()
        local.start()
    res_copy.start()

    q_copy.wait()
    for side, part_rows in enumerate(halves(q_vm)):
        part_rows = part_rows.astype(jnp.bfloat16)
        for h in range(kv_heads * group):
            q_stack[side, h // group, (h % group) * block:(h % group + 1) * block, :] = part_rows[
                :, h * HEAD_SIZE:(h + 1) * HEAD_SIZE
            ]

    for distance in range(1, ns - 1):
        for chunk in (0, 1):
            forward_kv(chunk, distance)
    start_kv(3, 0)
    collect_kv((0, 1), range(1, ns))

    chunk_blocks = math.gcd(ns, 4)
    factor = math.log2(math.e) * HEAD_SIZE ** -0.5
    stack = group * block

    def attend(state, q, g, late, masked, own_id, at, blocks):
        chunk_keys = blocks * block
        lanes = slice(g * HEAD_SIZE, (g + 1) * HEAD_SIZE)
        base = 2 if late else 0
        k = kv[base, pl.ds(at, blocks), :, lanes].reshape(chunk_keys, HEAD_SIZE)
        v = kv[base + 1, pl.ds(at, blocks), :, lanes].reshape(chunk_keys, HEAD_SIZE)
        scores = lax.dot_general(
            q, k, (((1,), (1,)), ((), ())), preferred_element_type=jnp.float32
        ) * factor
        if masked:
            starts = []
            for j in range(blocks):
                a, b = order_ref[2 * (at + j)], order_ref[2 * (at + j) + 1]
                there = jnp.maximum(a, b) if late else jnp.minimum(a, b)
                gap = (own_id - there) * block
                lane = lax.broadcasted_iota(jnp.int32, (block, block), 1)
                row = lax.broadcasted_iota(jnp.int32, (block, block), 0)
                starts.append(jnp.where(lane - row <= gap, 0.0, MASKED))
            bias = starts[0] if blocks == 1 else jnp.concatenate(starts, axis=1)
            scores = (scores.reshape(group, block, chunk_keys) + bias[None]).reshape(
                stack, chunk_keys
            )
        top = jnp.max(scores, axis=1, keepdims=True)
        if state is None:
            weights = jnp.exp2(scores - top)
            total = jnp.sum(weights, axis=1, keepdims=True)
            value = jnp.dot(weights.astype(jnp.bfloat16), v, preferred_element_type=jnp.float32)
            return top, total, value
        old_top, old_total, old_value = state
        top = jnp.maximum(old_top, top)
        weights = jnp.exp2(scores - top)
        scale = jnp.exp2(old_top - top)
        total = old_total * scale + jnp.sum(weights, axis=1, keepdims=True)
        value = old_value * scale + jnp.dot(
            weights.astype(jnp.bfloat16), v, preferred_element_type=jnp.float32
        )
        return top, total, value

    def attend_all(state, q, g, late, masked, own_id):
        if ns == chunk_blocks:
            return attend(state, q, g, late, masked, own_id, 0, ns)
        if state is None:
            state = (
                jnp.full((stack, 1), MASKED, jnp.float32),
                jnp.zeros((stack, 1), jnp.float32),
                jnp.zeros((stack, HEAD_SIZE), jnp.float32),
            )
        return lax.fori_loop(
            0,
            ns // chunk_blocks,
            lambda i, s: attend(
                s, q, g, late, masked, own_id, i * chunk_blocks, chunk_blocks
            ),
            state,
        )

    def store_attention(side, g, state):
        _, total, value = state
        result = (value / total).astype(jnp.bfloat16)
        for h in range(group):
            column = (g * group + h) * HEAD_SIZE
            att[side, :, column:column + HEAD_SIZE] = result[h * block:(h + 1) * block, :]

    def att_copy(side, g):
        lanes = slice(g * group * HEAD_SIZE, (g + 1) * group * HEAD_SIZE)
        return pltpu.make_async_remote_copy(
            src_ref=att.at[side, :, lanes],
            dst_ref=peer_att.at[side, :, lanes],
            send_sem=att_send.at[side, g],
            recv_sem=att_recv.at[side, g],
            device_id={"head": sibling},
            device_id_type=MESH,
        )

    pieces = features // math.gcd(features, 256)
    piece_width = features // pieces

    def part_copy(side, step, piece):
        return pltpu.make_async_remote_copy(
            src_ref=part.at[side, step - 1, piece],
            dst_ref=part_in.at[side, step - 1, piece],
            send_sem=part_send.at[side, step - 1, piece],
            recv_sem=part_recv.at[side, step - 1, piece],
            device_id={"head": 2 * lax.rem(pair + step, pairs) + bit},
            device_id_type=MESH,
        )

    def own_part(side, owner, columns):
        return jnp.dot(att[side], w_own[owner, :, columns], preferred_element_type=jnp.float32)

    def peer_part(side, owner, columns):
        return jnp.dot(
            peer_att[side], w_peer[owner, :, columns], preferred_element_type=jnp.float32
        )

    def own_residual(side, columns):
        low = res_vm[:block, columns].astype(jnp.float32)
        high = res_vm[block:, columns].astype(jnp.float32)
        swap = jnp.full(low.shape, swapped, jnp.int32) != 0
        return jnp.where(swap, high, low) if side == 0 else jnp.where(swap, low, high)

    spans = [slice(i * piece_width, (i + 1) * piece_width) for i in range(pieces)]

    def project_side(side):
        owner = lax.rem(pair + 1, pairs)
        for columns in spans:
            ahead[:, columns] = own_part(side, owner, columns)
        for g in range(kv_heads):
            att_copy(side, g).wait_recv()
        for step in range(1, pairs):
            owner = lax.rem(pair + step, pairs)
            for piece, columns in enumerate(spans):
                own = ahead[:, columns] if step == 1 else own_part(side, owner, columns)
                part[side, step - 1, piece] = (own + peer_part(side, owner, columns)).astype(
                    jnp.bfloat16
                )
                part_copy(side, step, piece).start()
        for columns in spans:
            mixed[side, :, columns] = (
                own_part(side, pair, columns)
                + peer_part(side, pair, columns)
                + own_residual(side, columns)
            )

    def ssq_copy(side, step):
        return pltpu.make_async_remote_copy(
            src_ref=ssq.at[side],
            dst_ref=ssq_in.at[side, step - 1],
            send_sem=ssq_send.at[side, step - 1],
            recv_sem=ssq_recv.at[side, step - 1],
            device_id={"head": lax.rem(head + step, nh)},
            device_id_type=MESH,
        )

    def finish_side(side):
        squares = jnp.zeros((block, 128), jnp.float32)
        for piece, columns in enumerate(spans):
            total = mixed[side, :, columns]
            for step in range(1, pairs):
                part_copy(side, step, piece).wait_recv()
                total = total + part_in[side, step - 1, piece].astype(jnp.float32)
            mixed[side, :, columns] = total
            for lane in range(0, piece_width, 128):
                strip = total[:, lane:lane + 128]
                squares = squares + strip * strip
        row_sums = jnp.sum(jnp.transpose(squares), axis=0, keepdims=True)
        ssq[side] = jnp.broadcast_to(row_sums, (8, block))
        for step in range(1, nh):
            ssq_copy(side, step).start()
        mixed[side] = mixed[side] * gain_ref[...].astype(jnp.float32).reshape(1, features)

    def norm_side(side):
        total = ssq[side]
        for step in range(1, nh):
            ssq_copy(side, step).wait_recv()
            total = total + ssq_in[side, step - 1]
        inverse = lax.rsqrt(total / (nh * features) + NORM_EPSILON)
        column = jnp.transpose(jnp.broadcast_to(inverse[:1, :], (128, block)))[:, :1]
        return mixed[side] * column

    def keep_state(g, state):
        top, total, value = state
        acc[g] = value
        peak[g] = jnp.broadcast_to(top, (stack, 128))
        denom[g] = jnp.broadcast_to(total, (stack, 128))

    def kept_state(g):
        return peak[g][:, :1], denom[g][:, :1], acc[g]

    late_steps = list(range(1, ns - 1))
    for g in range(kv_heads):
        store_attention(0, g, attend_all(None, q_stack[0, g], g, False, True, early_id))
        att_copy(0, g).start()
    for g in range(kv_heads):
        keep_state(g, attend_all(None, q_stack[1, g], g, False, False, late_id))
    for distance in late_steps[:1]:
        for chunk in (2, 3):
            forward_kv(chunk, distance)
    for index in range(pairs):
        local, remote = w_copies(index)
        local.wait()
        remote.wait_recv()
    res_copy.wait()
    loads[2].wait()
    project_side(0)
    for distance in late_steps[1:]:
        for chunk in (2, 3):
            forward_kv(chunk, distance)
    split = ns == chunk_blocks and ns > 1
    if split:
        lower = seq < ns // 2
        begin, far = jnp.where(lower, 0, 1), jnp.where(lower, ns - 1, 0)
        collect_kv((2, 3), range(1, ns - 1))
        for g in range(kv_heads):
            keep_state(
                g, attend(kept_state(g), q_stack[1, g], g, True, True, late_id, begin, ns - 1)
            )
    collect_kv((2, 3), range(ns - 1, ns) if split else range(1, ns))
    for g in range(kv_heads):
        if split:
            state = attend(kept_state(g), q_stack[1, g], g, True, True, late_id, far, 1)
        else:
            state = attend_all(kept_state(g), q_stack[1, g], g, True, True, late_id)
        store_attention(1, g, state)
        att_copy(1, g).start()
    project_side(1)
    finish_side(0)
    mixed[0] = norm_side(0)
    finish_side(1)
    early_out, late_out = mixed[0], norm_side(1)
    swap = jnp.full(early_out.shape, swapped, jnp.int32) != 0
    out_ref[:block, :] = jnp.where(swap, late_out, early_out).astype(jnp.bfloat16)
    out_ref[block:, :] = jnp.where(swap, early_out, late_out).astype(jnp.bfloat16)

    for chunk in range(4):
        for distance in range(ns - 1):
            for direction in range(2):
                @pl.when(sends(direction, distance))
                def _():
                    kv_copy(direction, chunk, distance).wait_send()
    for index in range(pairs):
        w_copies(index)[1].wait_send()
    for side in range(2):
        for g in range(kv_heads):
            att_copy(side, g).wait_send()
        for step in range(1, pairs):
            for piece in range(pieces):
                part_copy(side, step, piece).wait_send()
        for step in range(1, nh):
            ssq_copy(side, step).wait_send()


def body(ns, nh, queries, keys, values, residual, weight, gain, order):
    rows, width = queries.shape
    block, kv_width = rows // 2, keys.shape[1]
    kv_heads = kv_width // HEAD_SIZE
    stack = (width // kv_width) * block
    features = residual.shape[1]
    pairs = nh // 2
    others = max(pairs - 1, 1)
    pieces = features // math.gcd(features, 256)
    vmem, hbm = pl.BlockSpec(memory_space=pltpu.VMEM), pl.BlockSpec(memory_space=pl.ANY)
    bf16, f32, dma = jnp.bfloat16, jnp.float32, pltpu.SemaphoreType.DMA
    return pl.pallas_call(
        functools.partial(kernel, ns, nh),
        out_shape=jax.ShapeDtypeStruct((rows, features), bf16),
        in_specs=[pl.BlockSpec(memory_space=pltpu.SMEM)] + [hbm] * 6,
        out_specs=vmem,
        scratch_shapes=[
            pltpu.VMEM((rows, kv_width), bf16),
            pltpu.VMEM((rows, kv_width), bf16),
            pltpu.VMEM((features,), bf16),
            pltpu.VMEM((rows, width), bf16),
            pltpu.VMEM((rows, features), bf16),
            pltpu.VMEM((2, kv_heads, stack, HEAD_SIZE), bf16),
            pltpu.VMEM((pairs, width, features), bf16),
            pltpu.VMEM((pairs, width, features), bf16),
            pltpu.VMEM((4, ns, block, kv_width), bf16),
            pltpu.VMEM((2, block, width), bf16),
            pltpu.VMEM((2, block, width), bf16),
            pltpu.VMEM((2, others, pieces, block, features // pieces), bf16),
            pltpu.VMEM((2, others, pieces, block, features // pieces), bf16),
            pltpu.VMEM((2, 8, block), f32),
            pltpu.VMEM((2, nh - 1, 8, block), f32),
            pltpu.VMEM((kv_heads, stack, HEAD_SIZE), f32),
            pltpu.VMEM((kv_heads, stack, 128), f32),
            pltpu.VMEM((kv_heads, stack, 128), f32),
            pltpu.VMEM((2, block, features), f32),
            pltpu.VMEM((block, features), f32),
            dma((3,)),
            dma((2 + pairs,)),
            dma((2, 4, ns)),
            dma((4, ns)),
            dma((pairs,)),
            dma((pairs,)),
            dma((2, kv_heads)),
            dma((2, kv_heads)),
            dma((2, others, pieces)),
            dma((2, others, pieces)),
            dma((2, nh - 1)),
            dma((2, nh - 1)),
        ],
        compiler_params=pltpu.CompilerParams(
            collective_id=0, has_side_effects=True, vmem_limit_bytes=40 * 1024 * 1024
        ),
    )(*[pltpu.with_memory_space_constraint(a, pltpu.HBM) for a in (order, keys, values, gain, queries, residual, weight)])


def solution(mesh):
    in_specs = (
        P(("rep", "seq"), "head"),
        P(("rep", "seq"), "head"),
        P(("rep", "seq"), "head"),
        P(("rep", "seq"), "head"),
        P("head", None),
        P("head"),
        P("rep"),
    )
    out_specs = P(("rep", "seq"), "head")
    ns, nh = mesh.shape["seq"], mesh.shape["head"]
    return jax.shard_map(
        functools.partial(body, ns, nh),
        mesh=mesh,
        in_specs=in_specs,
        out_specs=out_specs,
        check_vma=False,
    )
```

```python
import functools
import math

import jax
import jax.numpy as jnp
from jax import lax
from jax.experimental import pallas as pl
from jax.experimental.pallas import tpu as pltpu
from jax.sharding import PartitionSpec as P

MESH = pl.DeviceIdType.MESH
HEAD_SIZE = 128
NORM_EPSILON = 1e-05
MASKED = -1e30


def kernel(
    ns, nh, order_hbm, k_hbm, v_hbm, gain_hbm, q_hbm, res_hbm, w_hbm, out_ref,
    order_ref, k_ref, v_ref, gain_ref, q_vm, res_vm, q_stack, w_own, w_peer, kv, att, peer_att, part, part_in,
    ssq, ssq_in, acc, peak, denom, mixed, ahead, peer_kv,
    load_sem, local_sem, kv_send, kv_recv, peer_send, peer_recv, relay_send, w_send, w_recv, att_send, att_recv,
    part_send, part_recv, ssq_send, ssq_recv,
):
    seq, head = lax.axis_index("seq"), lax.axis_index("head")
    rows, width = q_vm.shape
    block = rows // 2
    kv_heads = k_ref.shape[1] // HEAD_SIZE
    group = width // k_ref.shape[1]
    features = res_vm.shape[1]
    pairs = nh // 2
    bit, pair = lax.rem(head, 2), head // 2
    sibling = head + 1 - 2 * bit
    keys = ns * block

    def drain(ref, sem):
        pltpu.make_async_copy(ref, ref, sem).wait()

    barrier = pltpu.get_barrier_semaphore()

    near = jnp.where(seq > 0, 1, 0) + jnp.where(seq < ns - 1, 1, 0)

    @pl.when(seq > 0)
    def _():
        pl.semaphore_signal(barrier, inc=1, device_id={"seq": seq - 1}, device_id_type=MESH)

    @pl.when(seq < ns - 1)
    def _():
        pl.semaphore_signal(barrier, inc=1, device_id={"seq": seq + 1}, device_id_type=MESH)

    for offset in (-1, 1):
        @pl.when(jnp.logical_and(bit == 1, jnp.logical_and(seq + offset >= 0, seq + offset < ns)))
        def _():
            pl.semaphore_signal(
                barrier,
                inc=1,
                device_id={"seq": seq + offset, "head": sibling},
                device_id_type=MESH,
            )

    for step in range(1, nh):
        pl.semaphore_signal(
            barrier, inc=1, device_id={"head": lax.rem(head + step, nh)}, device_id_type=MESH
        )
    order_copy = pltpu.make_async_copy(order_hbm, order_ref, load_sem.at[3])
    order_copy.start()
    q_copy = pltpu.make_async_copy(q_hbm, q_vm, local_sem.at[0])
    res_copy = pltpu.make_async_copy(res_hbm, res_vm, local_sem.at[1])
    loads = [
        pltpu.make_async_copy(source, target, load_sem.at[i])
        for i, (source, target) in enumerate(((k_hbm, k_ref), (v_hbm, v_ref), (gain_hbm, gain_ref)))
    ]
    for load in loads:
        load.start()
    q_copy.start()

    order_copy.wait()
    first, second = order_ref[2 * seq], order_ref[2 * seq + 1]
    early_id, late_id = jnp.minimum(first, second), jnp.maximum(first, second)
    swapped = jnp.where(first > second, 1, 0)

    def halves(ref):
        low, high = ref[:block, :].astype(jnp.float32), ref[block:, :].astype(jnp.float32)
        swap = jnp.full(low.shape, swapped, jnp.int32) != 0
        return jnp.where(swap, high, low), jnp.where(swap, low, high)

    for index, ref in ((0, k_ref), (1, v_ref)):
        loads[index].wait()
        early, late = halves(ref)
        kv[index, seq] = early.astype(jnp.bfloat16)
        kv[2 + index, seq] = late.astype(jnp.bfloat16)

    pl.semaphore_wait(barrier, near * (2 - bit) + nh - 1)

    def kv_copy(direction, chunk, distance):
        piece = seq - distance if direction == 0 else seq + distance
        target = seq + 1 if direction == 0 else seq - 1
        return pltpu.make_async_remote_copy(
            src_ref=kv.at[chunk, piece],
            dst_ref=kv.at[chunk, piece],
            send_sem=kv_send.at[direction, distance],
            recv_sem=kv_recv.at[chunk, piece],
            device_id={"seq": target},
            device_id_type=MESH,
        )

    def sends(direction, distance):
        if direction == 0:
            return jnp.logical_and(seq >= distance, seq < ns - 1)
        return jnp.logical_and(seq + distance <= ns - 1, seq > 0)

    def arrives(direction, distance):
        return seq >= distance if direction == 0 else seq + distance <= ns - 1

    def cross_copy(direction, chunk):
        return pltpu.make_async_remote_copy(
            src_ref=kv.at[chunk, seq],
            dst_ref=peer_kv.at[chunk, seq],
            send_sem=kv_send.at[direction, 0],
            recv_sem=peer_recv.at[chunk, seq],
            device_id={"seq": seq + 1 if direction == 0 else seq - 1, "head": sibling},
            device_id_type=MESH,
        )

    def peer_copy(direction, chunk, distance, origin=None):
        origin = distance if origin is None else origin
        piece = seq - origin if direction == 0 else seq + origin
        return pltpu.make_async_remote_copy(
            src_ref=peer_kv.at[chunk, piece],
            dst_ref=peer_kv.at[chunk, piece],
            send_sem=peer_send.at[direction, distance - 1],
            recv_sem=peer_recv.at[chunk, piece],
            device_id={"seq": seq + 1 if direction == 0 else seq - 1},
            device_id_type=MESH,
        )

    def landed(direction, chunk, distance):
        return peer_copy(direction, chunk, min(distance, max(ns - 2, 1)), distance)

    def relay_copy(direction, chunk, distance):
        piece = seq - distance if direction == 0 else seq + distance
        return pltpu.make_async_remote_copy(
            src_ref=peer_kv.at[chunk, piece],
            dst_ref=kv.at[chunk, piece],
            send_sem=relay_send,
            recv_sem=kv_recv.at[chunk, piece],
            device_id={"head": sibling},
            device_id_type=MESH,
        )

    def start_kv(chunk):
        for direction in (1, 0):
            @pl.when(sends(direction, 0))
            def _():
                if chunk < 2:
                    @pl.when(bit == 0)
                    def _():
                        cross_copy(direction, chunk).start()

                    @pl.when(bit == 1)
                    def _():
                        kv_copy(direction, chunk, 0).start()
                else:
                    kv_copy(direction, chunk, 0).start()

    def passes(direction, chunk, distance):
        if distance >= ns - 1:
            return None
        condition = sends(direction, distance)
        return jnp.logical_and(condition, bit == 1) if chunk < 2 else condition

    def beside(direction):
        return seq == (1 if direction == 0 else ns - 2)

    def forward_kv(chunk, distance, edges=None):
        for direction in (1, 0):
            condition = passes(direction, chunk, distance)
            if edges is not None:
                chosen = beside(direction) if edges else jnp.logical_not(beside(direction))
                condition = jnp.logical_and(condition, chosen)

            @pl.when(condition)
            def _():
                kv_copy(direction, chunk, distance).wait_recv()
                kv_copy(direction, chunk, distance).start()

    def relay_kv(chunk, distance):
        for direction in (1, 0):
            @pl.when(jnp.logical_and(bit == 1, arrives(direction, distance)))
            def _():
                landed(direction, chunk, distance).wait_recv()
                if distance < ns - 1:
                    @pl.when(sends(direction, distance))
                    def _():
                        peer_copy(direction, chunk, distance).start()
                relay_copy(direction, chunk, distance).start()

    def collect_kv(chunks, distances):
        for distance in distances:
            for chunk in chunks:
                for direction in (1, 0):
                    condition = arrives(direction, distance)
                    passed = passes(direction, chunk, distance)
                    if passed is not None:
                        condition = jnp.logical_and(condition, jnp.logical_not(passed))

                    @pl.when(condition)
                    def _():
                        kv_copy(direction, chunk, distance).wait_recv()

    edge = jnp.logical_or(seq == 0, seq == ns - 1)
    for chunk in (0, 1, 2):
        start_kv(chunk)

    @pl.when(edge)
    def _():
        start_kv(3)

    def w_local(index):
        mine = pl.ds(pl.multiple_of((2 * index + bit) * features, 128), features)
        return pltpu.make_async_copy(w_hbm.at[:, mine], w_own.at[index], local_sem.at[2])

    slices = 4
    depth = width // slices

    def w_remote(number):
        index, rows_from = number // slices, number % slices * depth
        theirs = pl.ds(pl.multiple_of((2 * index + 1 - bit) * features, 128), features)
        return pltpu.make_async_remote_copy(
            src_ref=w_hbm.at[rows_from:rows_from + depth, theirs],
            dst_ref=w_peer.at[index, rows_from:rows_from + depth, :],
            send_sem=w_send,
            recv_sem=w_recv,
            device_id={"head": sibling},
            device_id_type=MESH,
        )

    w_pieces = list(range(pairs * slices))
    at_once = 2

    def w_next(count):
        for _ in range(min(count, len(w_pieces))):
            w_remote(w_pieces.pop(0)).start()

    for index in range(pairs):
        w_local(index).start()
    w_next(at_once)
    res_copy.start()

    q_copy.wait()
    for side, part_rows in enumerate(halves(q_vm)):
        part_rows = part_rows.astype(jnp.bfloat16)
        for h in range(kv_heads * group):
            q_stack[side, h // group, (h % group) * block:(h % group + 1) * block, :] = part_rows[
                :, h * HEAD_SIZE:(h + 1) * HEAD_SIZE
            ]

    for distance in range(1, ns):
        for chunk in (0, 1):
            relay_kv(chunk, distance)
            if distance < ns - 1:
                forward_kv(chunk, distance)
            w_next(1)
        if distance == max(ns - 2, 1):
            @pl.when(jnp.logical_not(edge))
            def _():
                start_kv(3)
    if ns > 2:
        for chunk in (2, 3):
            forward_kv(chunk, 1, edges=True)
    w_next(len(w_pieces))
    collect_kv((0, 1), range(1, ns))

    chunk_blocks = math.gcd(ns, 4)
    factor = math.log2(math.e) * HEAD_SIZE ** -0.5
    stack = group * block

    def weigh(state, q, g, late, masked, own_id, at, blocks):
        chunk_keys = blocks * block
        lanes = slice(g * HEAD_SIZE, (g + 1) * HEAD_SIZE)
        k = kv[2 if late else 0, pl.ds(at, blocks), :, lanes].reshape(chunk_keys, HEAD_SIZE)
        scores = lax.dot_general(
            q, k, (((1,), (1,)), ((), ())), preferred_element_type=jnp.float32
        ) * factor
        if masked:
            starts = []
            for j in range(blocks):
                a, b = order_ref[2 * (at + j)], order_ref[2 * (at + j) + 1]
                there = jnp.maximum(a, b) if late else jnp.minimum(a, b)
                gap = (own_id - there) * block
                lane = lax.broadcasted_iota(jnp.int32, (block, block), 1)
                row = lax.broadcasted_iota(jnp.int32, (block, block), 0)
                starts.append(jnp.where(lane - row <= gap, 0.0, MASKED))
            bias = starts[0] if blocks == 1 else jnp.concatenate(starts, axis=1)
            scores = (scores.reshape(group, block, chunk_keys) + bias[None]).reshape(
                stack, chunk_keys
            )
        top = jnp.max(scores, axis=1, keepdims=True)
        if state is None:
            weights = jnp.exp2(scores - top)
            return top, jnp.sum(weights, axis=1, keepdims=True), weights.astype(jnp.bfloat16), None
        old_top, old_total, old_value = state
        top = jnp.maximum(old_top, top)
        weights = jnp.exp2(scores - top)
        scale = jnp.exp2(old_top - top)
        total = old_total * scale + jnp.sum(weights, axis=1, keepdims=True)
        return top, total, weights.astype(jnp.bfloat16), old_value * scale

    def gather_values(weighed, g, late, at, blocks):
        top, total, weights, value = weighed
        lanes = slice(g * HEAD_SIZE, (g + 1) * HEAD_SIZE)
        v = kv[3 if late else 1, pl.ds(at, blocks), :, lanes].reshape(blocks * block, HEAD_SIZE)
        fresh = jnp.dot(weights, v, preferred_element_type=jnp.float32)
        return top, total, fresh if value is None else value + fresh

    def attend(state, q, g, late, masked, own_id, at, blocks):
        weighed = weigh(state, q, g, late, masked, own_id, at, blocks)
        return gather_values(weighed, g, late, at, blocks)

    def attend_all(state, q, g, late, masked, own_id):
        if ns == chunk_blocks:
            return attend(state, q, g, late, masked, own_id, 0, ns)
        if state is None:
            state = (
                jnp.full((stack, 1), MASKED, jnp.float32),
                jnp.zeros((stack, 1), jnp.float32),
                jnp.zeros((stack, HEAD_SIZE), jnp.float32),
            )
        return lax.fori_loop(
            0,
            ns // chunk_blocks,
            lambda i, s: attend(
                s, q, g, late, masked, own_id, i * chunk_blocks, chunk_blocks
            ),
            state,
        )

    def store_attention(side, g, state):
        _, total, value = state
        result = (value * (1.0 / total)).astype(jnp.bfloat16)
        for h in range(group):
            column = (g * group + h) * HEAD_SIZE
            att[side, :, column:column + HEAD_SIZE] = result[h * block:(h + 1) * block, :]

    def att_copy(side, g):
        lanes = slice(g * group * HEAD_SIZE, (g + 1) * group * HEAD_SIZE)
        return pltpu.make_async_remote_copy(
            src_ref=att.at[side, :, lanes],
            dst_ref=peer_att.at[side, :, lanes],
            send_sem=att_send,
            recv_sem=att_recv.at[side],
            device_id={"head": sibling},
            device_id_type=MESH,
        )

    pieces = features // math.gcd(features, 256)
    piece_width = features // pieces

    def part_copy(side, step, piece):
        return pltpu.make_async_remote_copy(
            src_ref=part.at[side, step - 1, piece],
            dst_ref=part_in.at[side, step - 1, piece],
            send_sem=part_send,
            recv_sem=part_recv.at[side, step - 1, piece],
            device_id={"head": 2 * lax.rem(pair + step, pairs) + bit},
            device_id_type=MESH,
        )

    def own_part(side, owner, columns):
        return jnp.dot(att[side], w_own[owner, :, columns], preferred_element_type=jnp.float32)

    def peer_part(side, owner, columns):
        return jnp.dot(
            peer_att[side], w_peer[owner, :, columns], preferred_element_type=jnp.float32
        )

    def own_residual(side, columns):
        low = res_vm[:block, columns].astype(jnp.float32)
        high = res_vm[block:, columns].astype(jnp.float32)
        swap = jnp.full(low.shape, swapped, jnp.int32) != 0
        return jnp.where(swap, high, low) if side == 0 else jnp.where(swap, low, high)

    spans = [slice(i * piece_width, (i + 1) * piece_width) for i in range(pieces)]

    def project_side(side):
        owner = lax.rem(pair + 1, pairs)
        for columns in spans:
            ahead[:, columns] = own_part(side, owner, columns)
        drain(peer_att.at[side], att_recv.at[side])
        for step in range(1, pairs):
            owner = lax.rem(pair + step, pairs)
            for piece, columns in enumerate(spans):
                own = ahead[:, columns] if step == 1 else own_part(side, owner, columns)
                part[side, step - 1, piece] = (own + peer_part(side, owner, columns)).astype(
                    jnp.bfloat16
                )
                part_copy(side, step, piece).start()
        for columns in spans:
            mixed[side, :, columns] = (
                own_part(side, pair, columns)
                + peer_part(side, pair, columns)
                + own_residual(side, columns)
            )

    def ssq_copy(side, step):
        return pltpu.make_async_remote_copy(
            src_ref=ssq.at[side],
            dst_ref=ssq_in.at[side, step - 1],
            send_sem=ssq_send,
            recv_sem=ssq_recv.at[side],
            device_id={"head": lax.rem(head + step, nh)},
            device_id_type=MESH,
        )

    def finish_side(side):
        squares = jnp.zeros((block, 128), jnp.float32)
        for piece, columns in enumerate(spans):
            total = mixed[side, :, columns]
            for step in range(1, pairs):
                part_copy(side, step, piece).wait_recv()
                total = total + part_in[side, step - 1, piece].astype(jnp.float32)
            mixed[side, :, columns] = total
            for lane in range(0, piece_width, 128):
                strip = total[:, lane:lane + 128]
                squares = squares + strip * strip
        row_sums = jnp.sum(jnp.transpose(squares), axis=0, keepdims=True)
        ssq[side] = jnp.broadcast_to(row_sums, (8, block))
        for step in range(1, nh):
            ssq_copy(side, step).start()
        mixed[side] = mixed[side] * gain_ref[...].astype(jnp.float32).reshape(1, features)

    def norm_side(side):
        drain(ssq_in.at[side], ssq_recv.at[side])
        total = ssq[side]
        for step in range(1, nh):
            total = total + ssq_in[side, step - 1]
        inverse = lax.rsqrt(total / (nh * features) + NORM_EPSILON)
        column = jnp.transpose(jnp.broadcast_to(inverse[:1, :], (128, block)))[:, :1]
        return mixed[side] * column

    def keep_state(g, state):
        top, total, value = state
        acc[g] = value
        peak[g] = jnp.broadcast_to(top, (stack, 128))
        denom[g] = jnp.broadcast_to(total, (stack, 128))

    def kept_state(g):
        return peak[g][:, :1], denom[g][:, :1], acc[g]

    late_steps = list(range(1, ns - 1))
    for g in range(kv_heads):
        store_attention(0, g, attend_all(None, q_stack[0, g], g, False, True, early_id))
        att_copy(0, g).start()
    for g in range(kv_heads):
        keep_state(g, attend_all(None, q_stack[1, g], g, False, False, late_id))
    for distance in late_steps[:1]:
        for chunk in (2, 3):
            forward_kv(chunk, distance, edges=False)
    drain(w_own, local_sem.at[2])
    drain(w_peer, w_recv)
    res_copy.wait()
    loads[2].wait()
    project_side(0)
    for distance in late_steps[1:]:
        for chunk in (2, 3):
            forward_kv(chunk, distance)
    split = ns == chunk_blocks and ns > 1
    if split:
        lower = seq < ns // 2
        begin, far = jnp.where(lower, 0, 1), jnp.where(lower, ns - 1, 0)
        collect_kv((2, 3), range(1, ns - 1))
        for g in range(kv_heads):
            keep_state(
                g, attend(kept_state(g), q_stack[1, g], g, True, True, late_id, begin, ns - 1)
            )
    if split:
        collect_kv((2,), range(ns - 1, ns))
        weighed = [
            weigh(kept_state(g), q_stack[1, g], g, True, True, late_id, far, 1)
            for g in range(kv_heads)
        ]
        collect_kv((3,), range(ns - 1, ns))
    else:
        collect_kv((2, 3), range(1, ns))
    for g in range(kv_heads):
        if split:
            state = gather_values(weighed[g], g, True, far, 1)
        else:
            state = attend_all(kept_state(g), q_stack[1, g], g, True, True, late_id)
        store_attention(1, g, state)
        att_copy(1, g).start()
    project_side(1)
    finish_side(0)
    finish_side(1)
    mixed[0] = norm_side(0)
    early_out, late_out = mixed[0], norm_side(1)
    swap = jnp.full(early_out.shape, swapped, jnp.int32) != 0
    out_ref[:block, :] = jnp.where(swap, late_out, early_out).astype(jnp.bfloat16)
    out_ref[block:, :] = jnp.where(swap, early_out, late_out).astype(jnp.bfloat16)

    for distance in range(ns - 1):
        for direction in range(2):
            @pl.when(sends(direction, distance))
            def _():
                if distance == 0:
                    drain(kv.at[:, seq], kv_send.at[direction, distance])
                else:
                    @pl.when(bit == 0)
                    def _():
                        drain(kv.at[2:, seq], kv_send.at[direction, distance])

                    @pl.when(bit == 1)
                    def _():
                        drain(kv.at[:, seq], kv_send.at[direction, distance])
                        drain(peer_kv.at[:, seq], peer_send.at[direction, distance - 1])

    @pl.when(bit == 1)
    def _():
        drain(kv.at[:2, : ns - 1], relay_send)
    drain(w_peer, w_send)
    drain(att, att_send)
    if pairs > 1:
        drain(part, part_send)
    drain(ssq_in, ssq_send)


def body(ns, nh, queries, keys, values, residual, weight, gain, order):
    rows, width = queries.shape
    block, kv_width = rows // 2, keys.shape[1]
    kv_heads = kv_width // HEAD_SIZE
    stack = (width // kv_width) * block
    features = residual.shape[1]
    pairs = nh // 2
    others = max(pairs - 1, 1)
    pieces = features // math.gcd(features, 256)
    vmem, hbm = pl.BlockSpec(memory_space=pltpu.VMEM), pl.BlockSpec(memory_space=pl.ANY)
    bf16, f32, dma = jnp.bfloat16, jnp.float32, pltpu.SemaphoreType.DMA
    return pl.pallas_call(
        functools.partial(kernel, ns, nh),
        out_shape=jax.ShapeDtypeStruct((rows, features), bf16),
        in_specs=[hbm] * 7,
        out_specs=vmem,
        scratch_shapes=[
            pltpu.SMEM(order.shape, jnp.int32),
            pltpu.VMEM((rows, kv_width), bf16),
            pltpu.VMEM((rows, kv_width), bf16),
            pltpu.VMEM((features,), bf16),
            pltpu.VMEM((rows, width), bf16),
            pltpu.VMEM((rows, features), bf16),
            pltpu.VMEM((2, kv_heads, stack, HEAD_SIZE), bf16),
            pltpu.VMEM((pairs, width, features), bf16),
            pltpu.VMEM((pairs, width, features), bf16),
            pltpu.VMEM((4, ns, block, kv_width), bf16),
            pltpu.VMEM((2, block, width), bf16),
            pltpu.VMEM((2, block, width), bf16),
            pltpu.VMEM((2, others, pieces, block, features // pieces), bf16),
            pltpu.VMEM((2, others, pieces, block, features // pieces), bf16),
            pltpu.VMEM((2, 8, block), f32),
            pltpu.VMEM((2, nh - 1, 8, block), f32),
            pltpu.VMEM((kv_heads, stack, HEAD_SIZE), f32),
            pltpu.VMEM((kv_heads, stack, 128), f32),
            pltpu.VMEM((kv_heads, stack, 128), f32),
            pltpu.VMEM((2, block, features), f32),
            pltpu.VMEM((block, features), f32),
            pltpu.VMEM((2, ns, block, kv_width), bf16),
            dma((4,)),
            dma((3,)),
            dma((2, ns - 1)),
            dma((4, ns)),
            dma((2, max(ns - 2, 1))),
            dma((2, ns)),
            dma(()),
            dma(()),
            dma(()),
            dma(()),
            dma((2,)),
            dma(()),
            dma((2, others, pieces)),
            dma(()),
            dma((2,)),
        ],
        compiler_params=pltpu.CompilerParams(
            collective_id=0, has_side_effects=True, vmem_limit_bytes=40 * 1024 * 1024
        ),
    )(*[pltpu.with_memory_space_constraint(a, pltpu.HBM) for a in (order, keys, values, gain, queries, residual, weight)])


def solution(mesh):
    in_specs = (
        P(("rep", "seq"), "head"),
        P(("rep", "seq"), "head"),
        P(("rep", "seq"), "head"),
        P(("rep", "seq"), "head"),
        P("head", None),
        P("head"),
        P("rep"),
    )
    out_specs = P(("rep", "seq"), "head")
    ns, nh = mesh.shape["seq"], mesh.shape["head"]
    return jax.shard_map(
        functools.partial(body, ns, nh),
        mesh=mesh,
        in_specs=in_specs,
        out_specs=out_specs,
        check_vma=False,
    )
```

```python
import functools
import math

import jax
import jax.numpy as jnp
from jax import lax
from jax.experimental import pallas as pl
from jax.experimental.pallas import tpu as pltpu
from jax.sharding import PartitionSpec as P

MESH = pl.DeviceIdType.MESH
HEAD_SIZE = 128
NORM_EPSILON = 1e-05
MASKED = -1e30


def kernel(
    ns, nh, order_hbm, k_hbm, v_hbm, gain_hbm, q_hbm, res_hbm, w_hbm, out_ref,
    order_ref, k_ref, v_ref, gain_ref, q_vm, res_vm, q_stack, w_own, w_peer, kv, att, peer_att, part, part_in,
    ssq, ssq_in, acc, peak, denom, mixed, ahead, peer_kv,
    load_sem, local_sem, kv_send, kv_recv, peer_send, peer_recv, relay_send, w_send, w_recv, att_send, att_recv,
    part_send, part_recv, ssq_send, ssq_recv,
):
    seq, head = lax.axis_index("seq"), lax.axis_index("head")
    rows, width = q_vm.shape
    block = rows // 2
    kv_heads = k_ref.shape[1] // HEAD_SIZE
    group = width // k_ref.shape[1]
    features = res_vm.shape[1]
    pairs = nh // 2
    bit, pair = lax.rem(head, 2), head // 2
    sibling = head + 1 - 2 * bit
    keys = ns * block

    def drain(ref, sem):
        pltpu.make_async_copy(ref, ref, sem).wait()

    barrier = pltpu.get_barrier_semaphore()

    near = jnp.where(seq > 0, 1, 0) + jnp.where(seq < ns - 1, 1, 0)

    @pl.when(seq > 0)
    def _():
        pl.semaphore_signal(barrier, inc=1, device_id={"seq": seq - 1}, device_id_type=MESH)

    @pl.when(seq < ns - 1)
    def _():
        pl.semaphore_signal(barrier, inc=1, device_id={"seq": seq + 1}, device_id_type=MESH)

    for offset in (-1, 1):
        @pl.when(jnp.logical_and(bit == 1, jnp.logical_and(seq + offset >= 0, seq + offset < ns)))
        def _():
            pl.semaphore_signal(
                barrier,
                inc=1,
                device_id={"seq": seq + offset, "head": sibling},
                device_id_type=MESH,
            )

    for step in range(1, nh):
        pl.semaphore_signal(
            barrier, inc=1, device_id={"head": lax.rem(head + step, nh)}, device_id_type=MESH
        )
    order_copy = pltpu.make_async_copy(order_hbm, order_ref, load_sem.at[3])
    order_copy.start()
    q_copy = pltpu.make_async_copy(q_hbm, q_vm, local_sem.at[0])
    res_copy = pltpu.make_async_copy(res_hbm, res_vm, local_sem.at[1])
    loads = [
        pltpu.make_async_copy(source, target, load_sem.at[i])
        for i, (source, target) in enumerate(((k_hbm, k_ref), (v_hbm, v_ref), (gain_hbm, gain_ref)))
    ]
    for load in loads:
        load.start()
    q_copy.start()

    order_copy.wait()
    first, second = order_ref[2 * seq], order_ref[2 * seq + 1]
    early_id, late_id = jnp.minimum(first, second), jnp.maximum(first, second)
    swapped = jnp.where(first > second, 1, 0)

    def halves(ref):
        low, high = ref[:block, :].astype(jnp.float32), ref[block:, :].astype(jnp.float32)
        swap = jnp.full(low.shape, swapped, jnp.int32) != 0
        return jnp.where(swap, high, low), jnp.where(swap, low, high)

    for index, ref in ((0, k_ref), (1, v_ref)):
        loads[index].wait()
        early, late = halves(ref)
        kv[index, seq] = early.astype(jnp.bfloat16)
        kv[2 + index, seq] = late.astype(jnp.bfloat16)

    pl.semaphore_wait(barrier, near * (2 - bit) + nh - 1)

    def kv_copy(direction, chunk, distance):
        piece = seq - distance if direction == 0 else seq + distance
        target = seq + 1 if direction == 0 else seq - 1
        return pltpu.make_async_remote_copy(
            src_ref=kv.at[chunk, piece],
            dst_ref=kv.at[chunk, piece],
            send_sem=kv_send.at[direction, distance],
            recv_sem=kv_recv.at[chunk, piece],
            device_id={"seq": target},
            device_id_type=MESH,
        )

    def sends(direction, distance):
        if direction == 0:
            return jnp.logical_and(seq >= distance, seq < ns - 1)
        return jnp.logical_and(seq + distance <= ns - 1, seq > 0)

    def arrives(direction, distance):
        return seq >= distance if direction == 0 else seq + distance <= ns - 1

    def cross_copy(direction, chunk):
        return pltpu.make_async_remote_copy(
            src_ref=kv.at[chunk, seq],
            dst_ref=peer_kv.at[chunk, seq],
            send_sem=kv_send.at[direction, 0],
            recv_sem=peer_recv.at[chunk, seq],
            device_id={"seq": seq + 1 if direction == 0 else seq - 1, "head": sibling},
            device_id_type=MESH,
        )

    def peer_copy(direction, chunk, distance, origin=None):
        origin = distance if origin is None else origin
        piece = seq - origin if direction == 0 else seq + origin
        return pltpu.make_async_remote_copy(
            src_ref=peer_kv.at[chunk, piece],
            dst_ref=peer_kv.at[chunk, piece],
            send_sem=peer_send.at[direction, distance - 1],
            recv_sem=peer_recv.at[chunk, piece],
            device_id={"seq": seq + 1 if direction == 0 else seq - 1},
            device_id_type=MESH,
        )

    def landed(direction, chunk, distance):
        return peer_copy(direction, chunk, min(distance, max(ns - 2, 1)), distance)

    def relay_copy(direction, chunk, distance):
        piece = seq - distance if direction == 0 else seq + distance
        return pltpu.make_async_remote_copy(
            src_ref=peer_kv.at[chunk, piece],
            dst_ref=kv.at[chunk, piece],
            send_sem=relay_send,
            recv_sem=kv_recv.at[chunk, piece],
            device_id={"head": sibling},
            device_id_type=MESH,
        )

    def start_kv(chunk):
        for direction in (1, 0):
            @pl.when(sends(direction, 0))
            def _():
                if chunk < 2:
                    @pl.when(bit == 0)
                    def _():
                        cross_copy(direction, chunk).start()

                    @pl.when(bit == 1)
                    def _():
                        kv_copy(direction, chunk, 0).start()
                else:
                    kv_copy(direction, chunk, 0).start()

    def passes(direction, chunk, distance):
        if distance >= ns - 1:
            return None
        condition = sends(direction, distance)
        return jnp.logical_and(condition, bit == 1) if chunk < 2 else condition

    def beside(direction):
        return seq == (1 if direction == 0 else ns - 2)

    def forward_kv(chunk, distance, edges=None):
        for direction in (1, 0):
            condition = passes(direction, chunk, distance)
            if edges is not None:
                chosen = beside(direction) if edges else jnp.logical_not(beside(direction))
                condition = jnp.logical_and(condition, chosen)

            @pl.when(condition)
            def _():
                kv_copy(direction, chunk, distance).wait_recv()
                kv_copy(direction, chunk, distance).start()

    def relay_kv(chunk, distance):
        for direction in (1, 0):
            @pl.when(jnp.logical_and(bit == 1, arrives(direction, distance)))
            def _():
                landed(direction, chunk, distance).wait_recv()
                if distance < ns - 1:
                    @pl.when(sends(direction, distance))
                    def _():
                        peer_copy(direction, chunk, distance).start()
                relay_copy(direction, chunk, distance).start()

    def collect_kv(chunks, distances):
        for distance in distances:
            for chunk in chunks:
                for direction in (1, 0):
                    condition = arrives(direction, distance)
                    passed = passes(direction, chunk, distance)
                    if passed is not None:
                        condition = jnp.logical_and(condition, jnp.logical_not(passed))

                    @pl.when(condition)
                    def _():
                        kv_copy(direction, chunk, distance).wait_recv()

    edge = jnp.logical_or(seq == 0, seq == ns - 1)
    for chunk in (0, 1, 2):
        start_kv(chunk)

    @pl.when(edge)
    def _():
        start_kv(3)

    def w_local(index):
        mine = pl.ds(pl.multiple_of((2 * index + bit) * features, 128), features)
        return pltpu.make_async_copy(w_hbm.at[:, mine], w_own.at[index], local_sem.at[2])

    slices = 4
    depth = width // slices

    def w_remote(number):
        index, rows_from = number // slices, number % slices * depth
        theirs = pl.ds(pl.multiple_of((2 * index + 1 - bit) * features, 128), features)
        return pltpu.make_async_remote_copy(
            src_ref=w_hbm.at[rows_from:rows_from + depth, theirs],
            dst_ref=w_peer.at[index, rows_from:rows_from + depth, :],
            send_sem=w_send,
            recv_sem=w_recv,
            device_id={"head": sibling},
            device_id_type=MESH,
        )

    w_pieces = list(range(pairs * slices))
    at_once = 4

    def w_next(count):
        for _ in range(min(count, len(w_pieces))):
            number = w_pieces.pop(0)

            @pl.when(bit == 1)
            def _():
                w_remote(number).start()

    for index in range(pairs):
        w_local(index).start()

    @pl.when(bit == 0)
    def _():
        for number in w_pieces:
            w_remote(number).start()

    w_next(at_once)
    res_copy.start()

    q_copy.wait()
    for side, part_rows in enumerate(halves(q_vm)):
        part_rows = part_rows.astype(jnp.bfloat16)
        for h in range(kv_heads * group):
            q_stack[side, h // group, (h % group) * block:(h % group + 1) * block, :] = part_rows[
                :, h * HEAD_SIZE:(h + 1) * HEAD_SIZE
            ]

    def pass_early(distance):
        for chunk in (0, 1):
            relay_kv(chunk, distance)
            if distance < ns - 1:
                forward_kv(chunk, distance)
            w_next(1)

    for distance in range(1, max(ns - 1, 2)):
        pass_early(distance)

    @pl.when(jnp.logical_not(edge))
    def _():
        start_kv(3)

    if ns > 2:
        forward_kv(2, 1)
        forward_kv(3, 1, edges=True)

    chunk_blocks = math.gcd(ns, 4)
    factor = math.log2(math.e) * HEAD_SIZE ** -0.5
    stack = group * block

    def weigh(state, q, g, late, masked, own_id, at, blocks):
        chunk_keys = blocks * block
        lanes = slice(g * HEAD_SIZE, (g + 1) * HEAD_SIZE)
        k = kv[2 if late else 0, pl.ds(at, blocks), :, lanes].reshape(chunk_keys, HEAD_SIZE)
        scores = lax.dot_general(
            q, k, (((1,), (1,)), ((), ())), preferred_element_type=jnp.float32
        ) * factor
        if masked:
            starts = []
            for j in range(blocks):
                a, b = order_ref[2 * (at + j)], order_ref[2 * (at + j) + 1]
                there = jnp.maximum(a, b) if late else jnp.minimum(a, b)
                gap = (own_id - there) * block
                lane = lax.broadcasted_iota(jnp.int32, (block, block), 1)
                row = lax.broadcasted_iota(jnp.int32, (block, block), 0)
                starts.append(jnp.where(lane - row <= gap, 0.0, MASKED))
            bias = starts[0] if blocks == 1 else jnp.concatenate(starts, axis=1)
            scores = (scores.reshape(group, block, chunk_keys) + bias[None]).reshape(
                stack, chunk_keys
            )
        top = jnp.broadcast_to(jnp.max(scores, axis=1, keepdims=True), (stack, HEAD_SIZE))
        if state is not None:
            top = jnp.maximum(state[0], top)
        weights = jnp.exp2(scores - jnp.tile(top, (1, chunk_keys // HEAD_SIZE)))
        total = jnp.broadcast_to(jnp.sum(weights, axis=1, keepdims=True), (stack, HEAD_SIZE))
        if state is None:
            return top, total, weights.astype(jnp.bfloat16), None
        scale = jnp.exp2(state[0] - top)
        total = state[1] * scale + total
        return top, total, weights.astype(jnp.bfloat16), state[2] * scale

    def gather_values(weighed, g, late, at, blocks):
        top, total, weights, value = weighed
        lanes = slice(g * HEAD_SIZE, (g + 1) * HEAD_SIZE)
        v = kv[3 if late else 1, pl.ds(at, blocks), :, lanes].reshape(blocks * block, HEAD_SIZE)
        fresh = jnp.dot(weights, v, preferred_element_type=jnp.float32)
        return top, total, fresh if value is None else value + fresh

    def attend(state, q, g, late, masked, own_id, at, blocks):
        weighed = weigh(state, q, g, late, masked, own_id, at, blocks)
        return gather_values(weighed, g, late, at, blocks)

    def attend_all(state, q, g, late, masked, own_id):
        if ns == chunk_blocks:
            return attend(state, q, g, late, masked, own_id, 0, ns)
        if state is None:
            state = (
                jnp.full((stack, HEAD_SIZE), MASKED, jnp.float32),
                jnp.zeros((stack, HEAD_SIZE), jnp.float32),
                jnp.zeros((stack, HEAD_SIZE), jnp.float32),
            )
        return lax.fori_loop(
            0,
            ns // chunk_blocks,
            lambda i, s: attend(
                s, q, g, late, masked, own_id, i * chunk_blocks, chunk_blocks
            ),
            state,
        )

    def store_attention(side, g, state):
        _, total, value = state
        result = (value * (1.0 / total)).astype(jnp.bfloat16)
        for h in range(group):
            column = (g * group + h) * HEAD_SIZE
            att[side, :, column:column + HEAD_SIZE] = result[h * block:(h + 1) * block, :]

    def att_copy(side, g):
        lanes = slice(g * group * HEAD_SIZE, (g + 1) * group * HEAD_SIZE)
        return pltpu.make_async_remote_copy(
            src_ref=att.at[side, :, lanes],
            dst_ref=peer_att.at[side, :, lanes],
            send_sem=att_send,
            recv_sem=att_recv.at[side],
            device_id={"head": sibling},
            device_id_type=MESH,
        )

    pieces = features // math.gcd(features, 256)
    piece_width = features // pieces

    def part_copy(side, step, piece):
        return pltpu.make_async_remote_copy(
            src_ref=part.at[side, step - 1, piece],
            dst_ref=part_in.at[side, step - 1, piece],
            send_sem=part_send,
            recv_sem=part_recv.at[side, step - 1, piece],
            device_id={"head": 2 * lax.rem(pair + step, pairs) + bit},
            device_id_type=MESH,
        )

    def own_part(side, owner, columns):
        return jnp.dot(att[side], w_own[owner, :, columns], preferred_element_type=jnp.float32)

    def peer_part(side, owner, columns):
        return jnp.dot(
            peer_att[side], w_peer[owner, :, columns], preferred_element_type=jnp.float32
        )

    def own_residual(side, columns):
        low = res_vm[:block, columns].astype(jnp.float32)
        high = res_vm[block:, columns].astype(jnp.float32)
        swap = jnp.full(low.shape, swapped, jnp.int32) != 0
        return jnp.where(swap, high, low) if side == 0 else jnp.where(swap, low, high)

    spans = [slice(i * piece_width, (i + 1) * piece_width) for i in range(pieces)]

    def lead(side, owner):
        for columns in spans:
            ahead[:, columns] = own_part(side, owner, columns)
        drain(peer_att.at[side], att_recv.at[side])

    def project_others(side, first):
        if first:
            lead(side, lax.rem(pair + 1, pairs))
        for step in range(1, pairs):
            owner = lax.rem(pair + step, pairs)
            for piece, columns in enumerate(spans):
                led = first and step == 1
                own = ahead[:, columns] if led else own_part(side, owner, columns)
                part[side, step - 1, piece] = (own + peer_part(side, owner, columns)).astype(
                    jnp.bfloat16
                )
                part_copy(side, step, piece).start()

    def project_mine(side, first):
        if first:
            lead(side, pair)
        for columns in spans:
            own = ahead[:, columns] if first else own_part(side, pair, columns)
            mixed[side, :, columns] = (
                own + peer_part(side, pair, columns) + own_residual(side, columns)
            )

    def project_side(side, stagger, between=None):
        def others_first():
            project_others(side, pairs > 1)
            if between is not None:
                between()
            project_mine(side, pairs == 1)

        if not stagger:
            others_first()
            return

        @pl.when(bit == 0)
        def _():
            others_first()

        @pl.when(bit == 1)
        def _():
            project_mine(side, True)
            project_others(side, False)

    def ssq_copy(side, step):
        return pltpu.make_async_remote_copy(
            src_ref=ssq.at[side],
            dst_ref=ssq_in.at[side, step - 1],
            send_sem=ssq_send,
            recv_sem=ssq_recv.at[side],
            device_id={"head": lax.rem(head + step, nh)},
            device_id_type=MESH,
        )

    def finish_side(side):
        squares = jnp.zeros((block, 128), jnp.float32)
        for piece, columns in enumerate(spans):
            total = mixed[side, :, columns]
            for step in range(1, pairs):
                part_copy(side, step, piece).wait_recv()
                total = total + part_in[side, step - 1, piece].astype(jnp.float32)
            mixed[side, :, columns] = total
            for lane in range(0, piece_width, 128):
                strip = total[:, lane:lane + 128]
                squares = squares + strip * strip
        row_sums = jnp.sum(jnp.transpose(squares), axis=0, keepdims=True)
        ssq[side] = jnp.broadcast_to(row_sums, (8, block))
        for step in range(1, nh):
            ssq_copy(side, step).start()
        mixed[side] = mixed[side] * gain_ref[...].astype(jnp.float32).reshape(1, features)

    def norm_side(side):
        drain(ssq_in.at[side], ssq_recv.at[side])
        total = ssq[side]
        for step in range(1, nh):
            total = total + ssq_in[side, step - 1]
        inverse = lax.rsqrt(total / (nh * features) + NORM_EPSILON)
        column = jnp.transpose(jnp.broadcast_to(inverse[:1, :], (128, block)))[:, :1]
        return mixed[side] * column

    def keep_state(g, state):
        top, total, value = state
        acc[g] = value
        peak[g] = top
        denom[g] = total

    def kept_state(g):
        return peak[g], denom[g], acc[g]

    late_steps = list(range(1, ns - 1))
    split = ns == chunk_blocks and ns > 2
    heads = range(kv_heads)
    if split:
        lower = seq < ns // 2
        begin, far = jnp.where(lower, 0, 1), jnp.where(lower, ns - 1, 0)
        collect_kv((0, 1), range(1, ns - 1))
        early = [
            attend(None, q_stack[0, g], g, False, True, early_id, begin, ns - 1) for g in heads
        ]
        for g in heads:
            keep_state(g, attend(None, q_stack[1, g], g, False, False, late_id, begin, ns - 1))
        relay_kv(0, ns - 1)
        w_next(1)
        collect_kv((0,), range(ns - 1, ns))
        weighed = [
            weigh(early[g], q_stack[0, g], g, False, True, early_id, far, 1) for g in heads
        ]
        relay_kv(1, ns - 1)
        w_next(len(w_pieces))
        collect_kv((1,), range(ns - 1, ns))
        for g in heads:
            store_attention(0, g, gather_values(weighed[g], g, False, far, 1))
            att_copy(0, g).start()
        forward_kv(3, 1, edges=False)
        for g in heads:
            keep_state(
                g, attend(kept_state(g), q_stack[1, g], g, False, False, late_id, far, 1)
            )
    else:
        if ns > 2:
            pass_early(ns - 1)
        w_next(len(w_pieces))
        collect_kv((0, 1), range(1, ns))
        for g in heads:
            store_attention(0, g, attend_all(None, q_stack[0, g], g, False, True, early_id))
            att_copy(0, g).start()
        for g in heads:
            keep_state(g, attend_all(None, q_stack[1, g], g, False, False, late_id))
    if ns > 2 and not split:
        forward_kv(3, 1, edges=False)
    if split:
        for distance in late_steps[1:]:
            for chunk in (2, 3):
                forward_kv(chunk, distance)
    drain(w_own, local_sem.at[2])
    drain(w_peer, w_recv)
    res_copy.wait()
    loads[2].wait()

    def late_forwards():
        if not split:
            for distance in late_steps[1:]:
                for chunk in (2, 3):
                    forward_kv(chunk, distance)

    project_side(0, False, late_forwards)
    if split:
        collect_kv((2, 3), range(1, ns - 1))
        for g in range(kv_heads):
            keep_state(
                g, attend(kept_state(g), q_stack[1, g], g, True, True, late_id, begin, ns - 1)
            )
    if split:
        collect_kv((2,), range(ns - 1, ns))
        weighed = [
            weigh(kept_state(g), q_stack[1, g], g, True, True, late_id, far, 1)
            for g in range(kv_heads)
        ]
        collect_kv((3,), range(ns - 1, ns))
    else:
        collect_kv((2, 3), range(1, ns))
    for g in range(kv_heads):
        if split:
            state = gather_values(weighed[g], g, True, far, 1)
        else:
            state = attend_all(kept_state(g), q_stack[1, g], g, True, True, late_id)
        store_attention(1, g, state)
        att_copy(1, g).start()
    project_side(1, False)
    finish_side(0)
    finish_side(1)
    mixed[0] = norm_side(0)
    early_out, late_out = mixed[0], norm_side(1)
    swap = jnp.full(early_out.shape, swapped, jnp.int32) != 0
    out_ref[:block, :] = jnp.where(swap, late_out, early_out).astype(jnp.bfloat16)
    out_ref[block:, :] = jnp.where(swap, early_out, late_out).astype(jnp.bfloat16)

    for distance in range(ns - 1):
        for direction in range(2):
            @pl.when(sends(direction, distance))
            def _():
                if distance == 0:
                    drain(kv.at[:, seq], kv_send.at[direction, distance])
                else:
                    @pl.when(bit == 0)
                    def _():
                        drain(kv.at[2:, seq], kv_send.at[direction, distance])

                    @pl.when(bit == 1)
                    def _():
                        drain(kv.at[:, seq], kv_send.at[direction, distance])
                        drain(peer_kv.at[:, seq], peer_send.at[direction, distance - 1])

    @pl.when(bit == 1)
    def _():
        drain(kv.at[:2, : ns - 1], relay_send)
    drain(w_peer, w_send)
    drain(att, att_send)
    if pairs > 1:
        drain(part, part_send)
    drain(ssq_in, ssq_send)


def body(ns, nh, queries, keys, values, residual, weight, gain, order):
    rows, width = queries.shape
    block, kv_width = rows // 2, keys.shape[1]
    kv_heads = kv_width // HEAD_SIZE
    stack = (width // kv_width) * block
    features = residual.shape[1]
    pairs = nh // 2
    others = max(pairs - 1, 1)
    pieces = features // math.gcd(features, 256)
    vmem, hbm = pl.BlockSpec(memory_space=pltpu.VMEM), pl.BlockSpec(memory_space=pl.ANY)
    bf16, f32, dma = jnp.bfloat16, jnp.float32, pltpu.SemaphoreType.DMA
    return pl.pallas_call(
        functools.partial(kernel, ns, nh),
        out_shape=jax.ShapeDtypeStruct((rows, features), bf16),
        in_specs=[hbm] * 7,
        out_specs=vmem,
        scratch_shapes=[
            pltpu.SMEM(order.shape, jnp.int32),
            pltpu.VMEM((rows, kv_width), bf16),
            pltpu.VMEM((rows, kv_width), bf16),
            pltpu.VMEM((features,), bf16),
            pltpu.VMEM((rows, width), bf16),
            pltpu.VMEM((rows, features), bf16),
            pltpu.VMEM((2, kv_heads, stack, HEAD_SIZE), bf16),
            pltpu.VMEM((pairs, width, features), bf16),
            pltpu.VMEM((pairs, width, features), bf16),
            pltpu.VMEM((4, ns, block, kv_width), bf16),
            pltpu.VMEM((2, block, width), bf16),
            pltpu.VMEM((2, block, width), bf16),
            pltpu.VMEM((2, others, pieces, block, features // pieces), bf16),
            pltpu.VMEM((2, others, pieces, block, features // pieces), bf16),
            pltpu.VMEM((2, 8, block), f32),
            pltpu.VMEM((2, nh - 1, 8, block), f32),
            pltpu.VMEM((kv_heads, stack, HEAD_SIZE), f32),
            pltpu.VMEM((kv_heads, stack, 128), f32),
            pltpu.VMEM((kv_heads, stack, 128), f32),
            pltpu.VMEM((2, block, features), f32),
            pltpu.VMEM((block, features), f32),
            pltpu.VMEM((2, ns, block, kv_width), bf16),
            dma((4,)),
            dma((3,)),
            dma((2, ns - 1)),
            dma((4, ns)),
            dma((2, max(ns - 2, 1))),
            dma((2, ns)),
            dma(()),
            dma(()),
            dma(()),
            dma(()),
            dma((2,)),
            dma(()),
            dma((2, others, pieces)),
            dma(()),
            dma((2,)),
        ],
        compiler_params=pltpu.CompilerParams(
            collective_id=0, has_side_effects=True, vmem_limit_bytes=40 * 1024 * 1024
        ),
    )(*[pltpu.with_memory_space_constraint(a, pltpu.HBM) for a in (order, keys, values, gain, queries, residual, weight)])


def solution(mesh):
    in_specs = (
        P(("rep", "seq"), "head"),
        P(("rep", "seq"), "head"),
        P(("rep", "seq"), "head"),
        P(("rep", "seq"), "head"),
        P("head", None),
        P("head"),
        P("rep"),
    )
    out_specs = P(("rep", "seq"), "head")
    ns, nh = mesh.shape["seq"], mesh.shape["head"]
    return jax.shard_map(
        functools.partial(body, ns, nh),
        mesh=mesh,
        in_specs=in_specs,
        out_specs=out_specs,
        check_vma=False,
    )
```

```python
import functools
import math

import jax
import jax.numpy as jnp
from jax import lax
from jax.experimental import pallas as pl
from jax.experimental.pallas import tpu as pltpu
from jax.sharding import PartitionSpec as P

MESH = pl.DeviceIdType.MESH
HEAD_SIZE = 128
NORM_EPSILON = 1e-05
MASKED = -1e30


def kernel(
    ns, nh, order_hbm, k_hbm, v_hbm, gain_hbm, q_hbm, res_hbm, w_hbm, out_ref,
    order_ref, k_ref, v_ref, gain_ref, q_vm, res_vm, q_stack, w_own, w_peer, kv, att, peer_att, part, part_in,
    ssq, ssq_in, acc, peak, denom, mixed, ahead, peer_kv,
    load_sem, local_sem, kv_send, kv_recv, peer_recv, relay_send, w_send, w_recv, att_send, att_recv,
    part_send, part_recv, ssq_send, ssq_recv,
):
    seq, head = lax.axis_index("seq"), lax.axis_index("head")
    rows, width = q_vm.shape
    block = rows // 2
    kv_heads = k_ref.shape[1] // HEAD_SIZE
    group = width // k_ref.shape[1]
    features = res_vm.shape[1]
    pairs = nh // 2
    bit, pair = lax.rem(head, 2), head // 2
    sibling = head + 1 - 2 * bit
    keys = ns * block

    def drain(ref, sem):
        pltpu.make_async_copy(ref, ref, sem).wait()

    barrier = pltpu.get_barrier_semaphore()

    near = jnp.where(seq > 0, 1, 0) + jnp.where(seq < ns - 1, 1, 0)

    @pl.when(seq > 0)
    def _():
        pl.semaphore_signal(barrier, inc=1, device_id={"seq": seq - 1}, device_id_type=MESH)

    @pl.when(seq < ns - 1)
    def _():
        pl.semaphore_signal(barrier, inc=1, device_id={"seq": seq + 1}, device_id_type=MESH)

    for offset in (-1, 1):
        @pl.when(jnp.logical_and(bit == 1, jnp.logical_and(seq + offset >= 0, seq + offset < ns)))
        def _():
            pl.semaphore_signal(
                barrier,
                inc=1,
                device_id={"seq": seq + offset, "head": sibling},
                device_id_type=MESH,
            )

    for step in range(1, nh):
        pl.semaphore_signal(
            barrier, inc=1, device_id={"head": lax.rem(head + step, nh)}, device_id_type=MESH
        )
    order_copy = pltpu.make_async_copy(order_hbm, order_ref, load_sem.at[3])
    order_copy.start()
    q_copy = pltpu.make_async_copy(q_hbm, q_vm, local_sem.at[0])
    res_copy = pltpu.make_async_copy(res_hbm, res_vm, local_sem.at[1])
    loads = [
        pltpu.make_async_copy(source, target, load_sem.at[i])
        for i, (source, target) in enumerate(((k_hbm, k_ref), (v_hbm, v_ref), (gain_hbm, gain_ref)))
    ]
    for load in loads:
        load.start()
    q_copy.start()

    order_copy.wait()
    first, second = order_ref[2 * seq], order_ref[2 * seq + 1]
    early_id, late_id = jnp.minimum(first, second), jnp.maximum(first, second)
    swapped = jnp.where(first > second, 1, 0)

    def halves(ref):
        low, high = ref[:block, :].astype(jnp.float32), ref[block:, :].astype(jnp.float32)
        swap = jnp.full(low.shape, swapped, jnp.int32) != 0
        return jnp.where(swap, high, low), jnp.where(swap, low, high)

    for index, ref in ((0, k_ref), (1, v_ref)):
        loads[index].wait()
        early, late = halves(ref)
        kv[index, seq] = early.astype(jnp.bfloat16)
        kv[2 + index, seq] = late.astype(jnp.bfloat16)

    pl.semaphore_wait(barrier, near * (2 - bit) + nh - 1)

    def kv_copy(direction, chunk, distance):
        piece = seq - distance if direction == 0 else seq + distance
        target = seq + 1 if direction == 0 else seq - 1
        return pltpu.make_async_remote_copy(
            src_ref=kv.at[chunk, piece],
            dst_ref=kv.at[chunk, piece],
            send_sem=kv_send.at[direction, distance],
            recv_sem=kv_recv.at[chunk, piece - direction],
            device_id={"seq": target},
            device_id_type=MESH,
        )

    def sends(direction, distance):
        if direction == 0:
            return jnp.logical_and(seq >= distance, seq < ns - 1)
        return jnp.logical_and(seq + distance <= ns - 1, seq > 0)

    def arrives(direction, distance):
        return seq >= distance if direction == 0 else seq + distance <= ns - 1

    def cross_copy(direction, chunk):
        return pltpu.make_async_remote_copy(
            src_ref=kv.at[chunk, seq],
            dst_ref=peer_kv.at[chunk, seq],
            send_sem=kv_send.at[direction, 0],
            recv_sem=peer_recv.at[chunk, seq - direction],
            device_id={"seq": seq + 1 if direction == 0 else seq - 1, "head": sibling},
            device_id_type=MESH,
        )

    def peer_copy(direction, chunk, distance, origin=None):
        origin = distance if origin is None else origin
        piece = seq - origin if direction == 0 else seq + origin
        return pltpu.make_async_remote_copy(
            src_ref=peer_kv.at[chunk, piece],
            dst_ref=peer_kv.at[chunk, piece],
            send_sem=kv_send.at[direction, distance],
            recv_sem=peer_recv.at[chunk, piece - direction],
            device_id={"seq": seq + 1 if direction == 0 else seq - 1},
            device_id_type=MESH,
        )

    def landed(direction, chunk, distance):
        return peer_copy(direction, chunk, min(distance, max(ns - 2, 1)), distance)

    def relay_copy(direction, chunk, distance):
        piece = seq - distance if direction == 0 else seq + distance
        return pltpu.make_async_remote_copy(
            src_ref=peer_kv.at[chunk, piece],
            dst_ref=kv.at[chunk, piece],
            send_sem=relay_send,
            recv_sem=kv_recv.at[chunk, piece - direction],
            device_id={"head": sibling},
            device_id_type=MESH,
        )

    def start_kv(chunk):
        for direction in (1, 0):
            @pl.when(sends(direction, 0))
            def _():
                if chunk < 2:
                    @pl.when(bit == 0)
                    def _():
                        cross_copy(direction, chunk).start()

                    @pl.when(bit == 1)
                    def _():
                        kv_copy(direction, chunk, 0).start()
                else:
                    kv_copy(direction, chunk, 0).start()

    def passes(direction, chunk, distance):
        if distance >= ns - 1:
            return None
        condition = sends(direction, distance)
        return jnp.logical_and(condition, bit == 1) if chunk < 2 else condition

    def beside(direction):
        return seq == (1 if direction == 0 else ns - 2)

    def forward_kv(chunk, distance, edges=None):
        for direction in (1, 0):
            condition = passes(direction, chunk, distance)
            if edges is not None:
                chosen = beside(direction) if edges else jnp.logical_not(beside(direction))
                condition = jnp.logical_and(condition, chosen)

            @pl.when(condition)
            def _():
                kv_copy(direction, chunk, distance).wait_recv()
                kv_copy(direction, chunk, distance).start()

    def relay_kv(chunk, distance):
        for direction in (1, 0):
            @pl.when(jnp.logical_and(bit == 1, arrives(direction, distance)))
            def _():
                landed(direction, chunk, distance).wait_recv()
                if distance < ns - 1:
                    @pl.when(sends(direction, distance))
                    def _():
                        peer_copy(direction, chunk, distance).start()
                relay_copy(direction, chunk, distance).start()

    def collect_kv(chunks, distances):
        for distance in distances:
            for chunk in chunks:
                for direction in (1, 0):
                    condition = arrives(direction, distance)
                    passed = passes(direction, chunk, distance)
                    if passed is not None:
                        condition = jnp.logical_and(condition, jnp.logical_not(passed))

                    @pl.when(condition)
                    def _():
                        kv_copy(direction, chunk, distance).wait_recv()

    edge = jnp.logical_or(seq == 0, seq == ns - 1)
    for chunk in (0, 1):
        start_kv(chunk)

    @pl.when(edge)
    def _():
        start_kv(2)
        start_kv(3)

    def w_local(index):
        mine = pl.ds(pl.multiple_of((2 * index + bit) * features, 128), features)
        return pltpu.make_async_copy(w_hbm.at[:, mine], w_own.at[index], local_sem.at[2])

    slices = 4
    depth = width // slices

    def w_remote(number):
        index, rows_from = number // slices, number % slices * depth
        theirs = pl.ds(pl.multiple_of((2 * index + 1 - bit) * features, 128), features)
        return pltpu.make_async_remote_copy(
            src_ref=w_hbm.at[rows_from:rows_from + depth, theirs],
            dst_ref=w_peer.at[index, rows_from:rows_from + depth, :],
            send_sem=w_send,
            recv_sem=w_recv,
            device_id={"head": sibling},
            device_id_type=MESH,
        )

    w_pieces = list(range(pairs * slices))
    at_once = 4

    def w_next(count):
        for _ in range(min(count, len(w_pieces))):
            number = w_pieces.pop(0)

            @pl.when(bit == 1)
            def _():
                w_remote(number).start()

    for index in range(pairs):
        w_local(index).start()

    @pl.when(bit == 0)
    def _():
        for number in w_pieces:
            w_remote(number).start()

    w_next(at_once)
    res_copy.start()

    q_copy.wait()
    for side, part_rows in enumerate(halves(q_vm)):
        part_rows = part_rows.astype(jnp.bfloat16)
        for h in range(kv_heads * group):
            q_stack[side, h // group, (h % group) * block:(h % group + 1) * block, :] = part_rows[
                :, h * HEAD_SIZE:(h + 1) * HEAD_SIZE
            ]

    def pass_early(distance):
        for chunk in (0, 1):
            relay_kv(chunk, distance)
            if distance < ns - 1:
                forward_kv(chunk, distance)
            w_next(1)

    for distance in range(1, max(ns - 1, 2)):
        pass_early(distance)

    @pl.when(jnp.logical_not(edge))
    def _():
        start_kv(2)
        start_kv(3)

    if ns > 2:
        forward_kv(2, 1)
        forward_kv(3, 1, edges=True)

    chunk_blocks = math.gcd(ns, 4)
    factor = math.log2(math.e) * HEAD_SIZE ** -0.5
    stack = group * block

    def weigh(state, q, g, late, masked, own_id, at, blocks):
        chunk_keys = blocks * block
        lanes = slice(g * HEAD_SIZE, (g + 1) * HEAD_SIZE)
        k = kv[2 if late else 0, pl.ds(at, blocks), :, lanes].reshape(chunk_keys, HEAD_SIZE)
        scores = lax.dot_general(
            q, k, (((1,), (1,)), ((), ())), preferred_element_type=jnp.float32
        ) * factor
        if masked:
            starts = []
            for j in range(blocks):
                a, b = order_ref[2 * (at + j)], order_ref[2 * (at + j) + 1]
                there = jnp.maximum(a, b) if late else jnp.minimum(a, b)
                gap = (own_id - there) * block
                lane = lax.broadcasted_iota(jnp.int32, (block, block), 1)
                row = lax.broadcasted_iota(jnp.int32, (block, block), 0)
                starts.append(jnp.where(lane - row <= gap, 0.0, MASKED))
            bias = starts[0] if blocks == 1 else jnp.concatenate(starts, axis=1)
            scores = (scores.reshape(group, block, chunk_keys) + bias[None]).reshape(
                stack, chunk_keys
            )
        top = jnp.broadcast_to(jnp.max(scores, axis=1, keepdims=True), (stack, HEAD_SIZE))
        if state is not None:
            top = jnp.maximum(state[0], top)
        weights = jnp.exp2(scores - jnp.tile(top, (1, chunk_keys // HEAD_SIZE)))
        total = jnp.broadcast_to(jnp.sum(weights, axis=1, keepdims=True), (stack, HEAD_SIZE))
        if state is None:
            return top, total, weights.astype(jnp.bfloat16), None
        scale = jnp.exp2(state[0] - top)
        total = state[1] * scale + total
        return top, total, weights.astype(jnp.bfloat16), state[2] * scale

    def gather_values(weighed, g, late, at, blocks):
        top, total, weights, value = weighed
        lanes = slice(g * HEAD_SIZE, (g + 1) * HEAD_SIZE)
        v = kv[3 if late else 1, pl.ds(at, blocks), :, lanes].reshape(blocks * block, HEAD_SIZE)
        fresh = jnp.dot(weights, v, preferred_element_type=jnp.float32)
        return top, total, fresh if value is None else value + fresh

    def attend(state, q, g, late, masked, own_id, at, blocks):
        weighed = weigh(state, q, g, late, masked, own_id, at, blocks)
        return gather_values(weighed, g, late, at, blocks)

    def attend_all(state, q, g, late, masked, own_id):
        if ns == chunk_blocks:
            return attend(state, q, g, late, masked, own_id, 0, ns)
        if state is None:
            state = (
                jnp.full((stack, HEAD_SIZE), MASKED, jnp.float32),
                jnp.zeros((stack, HEAD_SIZE), jnp.float32),
                jnp.zeros((stack, HEAD_SIZE), jnp.float32),
            )
        return lax.fori_loop(
            0,
            ns // chunk_blocks,
            lambda i, s: attend(
                s, q, g, late, masked, own_id, i * chunk_blocks, chunk_blocks
            ),
            state,
        )

    def store_attention(side, g, state):
        _, total, value = state
        result = (value * (1.0 / total)).astype(jnp.bfloat16)
        for h in range(group):
            column = (g * group + h) * HEAD_SIZE
            att[side, :, column:column + HEAD_SIZE] = result[h * block:(h + 1) * block, :]

    def att_copy(side, g):
        lanes = slice(g * group * HEAD_SIZE, (g + 1) * group * HEAD_SIZE)
        return pltpu.make_async_remote_copy(
            src_ref=att.at[side, :, lanes],
            dst_ref=peer_att.at[side, :, lanes],
            send_sem=att_send,
            recv_sem=att_recv.at[side],
            device_id={"head": sibling},
            device_id_type=MESH,
        )

    pieces = features // math.gcd(features, 512)
    piece_width = features // pieces

    def part_copy(side, step, piece):
        return pltpu.make_async_remote_copy(
            src_ref=part.at[side, step - 1, piece],
            dst_ref=part_in.at[side, step - 1, piece],
            send_sem=part_send,
            recv_sem=part_recv.at[step - 1, 0 if side == 0 else 1 + piece],
            device_id={"head": 2 * lax.rem(pair + step, pairs) + bit},
            device_id_type=MESH,
        )

    def own_part(side, owner, columns):
        return jnp.dot(att[side], w_own[owner, :, columns], preferred_element_type=jnp.float32)

    def peer_part(side, owner, columns):
        return jnp.dot(
            peer_att[side], w_peer[owner, :, columns], preferred_element_type=jnp.float32
        )

    def own_residual(side, columns):
        low = res_vm[:block, columns].astype(jnp.float32)
        high = res_vm[block:, columns].astype(jnp.float32)
        swap = jnp.full(low.shape, swapped, jnp.int32) != 0
        return jnp.where(swap, high, low) if side == 0 else jnp.where(swap, low, high)

    spans = [slice(i * piece_width, (i + 1) * piece_width) for i in range(pieces)]

    def lead(side, owner):
        for columns in spans:
            ahead[:, columns] = own_part(side, owner, columns)
        drain(peer_att.at[side], att_recv.at[side])

    def project_others(side, first):
        if first:
            lead(side, lax.rem(pair + 1, pairs))
        for step in range(1, pairs):
            owner = lax.rem(pair + step, pairs)
            for piece, columns in enumerate(spans):
                led = first and step == 1
                own = ahead[:, columns] if led else own_part(side, owner, columns)
                part[side, step - 1, piece] = (own + peer_part(side, owner, columns)).astype(
                    jnp.bfloat16
                )
                part_copy(side, step, piece).start()

    def project_mine(side, first):
        if first:
            lead(side, pair)
        for columns in spans:
            own = ahead[:, columns] if first else own_part(side, pair, columns)
            mixed[side, :, columns] = (
                own + peer_part(side, pair, columns) + own_residual(side, columns)
            )

    def project_side(side, stagger, between=None):
        def others_first():
            project_others(side, pairs > 1)
            if between is not None:
                between()
            project_mine(side, pairs == 1)

        if not stagger:
            others_first()
            return

        @pl.when(bit == 0)
        def _():
            others_first()

        @pl.when(bit == 1)
        def _():
            project_mine(side, True)
            project_others(side, False)

    def ssq_copy(side, step):
        return pltpu.make_async_remote_copy(
            src_ref=ssq.at[side],
            dst_ref=ssq_in.at[side, step - 1],
            send_sem=ssq_send,
            recv_sem=ssq_recv.at[side],
            device_id={"head": lax.rem(head + step, nh)},
            device_id_type=MESH,
        )

    def finish_side(side):
        squares = jnp.zeros((block, 128), jnp.float32)
        if side == 0:
            for step in range(1, pairs):
                drain(part_in.at[side, step - 1], part_recv.at[step - 1, 0])
        for piece, columns in enumerate(spans):
            total = mixed[side, :, columns]
            for step in range(1, pairs):
                if side == 1:
                    part_copy(side, step, piece).wait_recv()
                total = total + part_in[side, step - 1, piece].astype(jnp.float32)
            mixed[side, :, columns] = total
            for lane in range(0, piece_width, 128):
                strip = total[:, lane:lane + 128]
                squares = squares + strip * strip
        row_sums = jnp.sum(jnp.transpose(squares), axis=0, keepdims=True)
        ssq[side] = jnp.broadcast_to(row_sums, (8, block))
        for step in range(1, nh):
            ssq_copy(side, step).start()
        mixed[side] = mixed[side] * gain_ref[...].astype(jnp.float32).reshape(1, features)

    def norm_side(side):
        drain(ssq_in.at[side], ssq_recv.at[side])
        total = ssq[side]
        for step in range(1, nh):
            total = total + ssq_in[side, step - 1]
        inverse = lax.rsqrt(total / (nh * features) + NORM_EPSILON)
        column = jnp.transpose(jnp.broadcast_to(inverse[:1, :], (128, block)))[:, :1]
        return mixed[side] * column

    def keep_state(g, state):
        top, total, value = state
        acc[g] = value
        peak[g] = top
        denom[g] = total

    def kept_state(g):
        return peak[g], denom[g], acc[g]

    late_steps = list(range(1, ns - 1))
    split = ns == chunk_blocks and ns > 2
    heads = range(kv_heads)
    if split:
        lower = seq < ns // 2
        begin, far = jnp.where(lower, 0, 1), jnp.where(lower, ns - 1, 0)
        collect_kv((0, 1), range(1, ns - 1))
        early = [
            attend(None, q_stack[0, g], g, False, True, early_id, begin, ns - 1) for g in heads
        ]
        relay_kv(0, ns - 1)
        w_next(1)
        collect_kv((0,), range(ns - 1, ns))
        weighed = [
            weigh(early[g], q_stack[0, g], g, False, True, early_id, far, 1) for g in heads
        ]
        relay_kv(1, ns - 1)
        w_next(len(w_pieces))
        collect_kv((1,), range(ns - 1, ns))
        for g in heads:
            store_attention(0, g, gather_values(weighed[g], g, False, far, 1))
            att_copy(0, g).start()
        forward_kv(3, 1, edges=False)
        for g in heads:
            keep_state(g, attend_all(None, q_stack[1, g], g, False, False, late_id))
    else:
        if ns > 2:
            pass_early(ns - 1)
        w_next(len(w_pieces))
        collect_kv((0, 1), range(1, ns))
        for g in heads:
            store_attention(0, g, attend_all(None, q_stack[0, g], g, False, True, early_id))
            att_copy(0, g).start()
        for g in heads:
            keep_state(g, attend_all(None, q_stack[1, g], g, False, False, late_id))
    if ns > 2 and not split:
        forward_kv(3, 1, edges=False)
    if split:
        for distance in late_steps[1:]:
            for chunk in (2, 3):
                forward_kv(chunk, distance)
    drain(w_own, local_sem.at[2])
    drain(w_peer, w_recv)
    res_copy.wait()
    loads[2].wait()

    def late_forwards():
        if not split:
            for distance in late_steps[1:]:
                for chunk in (2, 3):
                    forward_kv(chunk, distance)

    project_side(0, False, late_forwards)
    if split:
        collect_kv((2, 3), range(1, ns - 1))
        for g in range(kv_heads):
            keep_state(
                g, attend(kept_state(g), q_stack[1, g], g, True, True, late_id, begin, ns - 1)
            )
    if split:
        collect_kv((2,), range(ns - 1, ns))
        weighed = [
            weigh(kept_state(g), q_stack[1, g], g, True, True, late_id, far, 1)
            for g in range(kv_heads)
        ]
        collect_kv((3,), range(ns - 1, ns))
    else:
        collect_kv((2, 3), range(1, ns))
    for g in range(kv_heads):
        if split:
            state = gather_values(weighed[g], g, True, far, 1)
        else:
            state = attend_all(kept_state(g), q_stack[1, g], g, True, True, late_id)
        store_attention(1, g, state)
        att_copy(1, g).start()
    project_side(1, False)
    finish_side(0)
    finish_side(1)
    mixed[0] = norm_side(0)
    early_out, late_out = mixed[0], norm_side(1)
    swap = jnp.full(early_out.shape, swapped, jnp.int32) != 0
    out_ref[:block, :] = jnp.where(swap, late_out, early_out).astype(jnp.bfloat16)
    out_ref[block:, :] = jnp.where(swap, early_out, late_out).astype(jnp.bfloat16)

    for distance in range(ns - 1):
        for direction in range(2):
            @pl.when(sends(direction, distance))
            def _():
                if distance == 0:
                    drain(kv.at[:, seq], kv_send.at[direction, distance])
                else:
                    @pl.when(bit == 0)
                    def _():
                        drain(kv.at[2:, seq], kv_send.at[direction, distance])

                    @pl.when(bit == 1)
                    def _():
                        drain(kv.at[:3, :2], kv_send.at[direction, distance])

    @pl.when(bit == 1)
    def _():
        drain(kv.at[:2, : ns - 1], relay_send)
    drain(w_peer, w_send)
    drain(att, att_send)
    if pairs > 1:
        drain(part, part_send)
    drain(ssq_in, ssq_send)


def body(ns, nh, queries, keys, values, residual, weight, gain, order):
    rows, width = queries.shape
    block, kv_width = rows // 2, keys.shape[1]
    kv_heads = kv_width // HEAD_SIZE
    stack = (width // kv_width) * block
    features = residual.shape[1]
    pairs = nh // 2
    others = max(pairs - 1, 1)
    pieces = features // math.gcd(features, 512)
    vmem, hbm = pl.BlockSpec(memory_space=pltpu.VMEM), pl.BlockSpec(memory_space=pl.ANY)
    bf16, f32, dma = jnp.bfloat16, jnp.float32, pltpu.SemaphoreType.DMA
    return pl.pallas_call(
        functools.partial(kernel, ns, nh),
        out_shape=jax.ShapeDtypeStruct((rows, features), bf16),
        in_specs=[hbm] * 7,
        out_specs=vmem,
        scratch_shapes=[
            pltpu.SMEM(order.shape, jnp.int32),
            pltpu.VMEM((rows, kv_width), bf16),
            pltpu.VMEM((rows, kv_width), bf16),
            pltpu.VMEM((features,), bf16),
            pltpu.VMEM((rows, width), bf16),
            pltpu.VMEM((rows, features), bf16),
            pltpu.VMEM((2, kv_heads, stack, HEAD_SIZE), bf16),
            pltpu.VMEM((pairs, width, features), bf16),
            pltpu.VMEM((pairs, width, features), bf16),
            pltpu.VMEM((4, ns, block, kv_width), bf16),
            pltpu.VMEM((2, block, width), bf16),
            pltpu.VMEM((2, block, width), bf16),
            pltpu.VMEM((2, others, pieces, block, features // pieces), bf16),
            pltpu.VMEM((2, others, pieces, block, features // pieces), bf16),
            pltpu.VMEM((2, 8, block), f32),
            pltpu.VMEM((2, nh - 1, 8, block), f32),
            pltpu.VMEM((kv_heads, stack, HEAD_SIZE), f32),
            pltpu.VMEM((kv_heads, stack, 128), f32),
            pltpu.VMEM((kv_heads, stack, 128), f32),
            pltpu.VMEM((2, block, features), f32),
            pltpu.VMEM((block, features), f32),
            pltpu.VMEM((2, ns, block, kv_width), bf16),
            dma((4,)),
            dma((3,)),
            dma((2, ns - 1)),
            dma((4, ns - 1)),
            dma((2, ns - 1)),
            dma(()),
            dma(()),
            dma(()),
            dma(()),
            dma((2,)),
            dma(()),
            dma((others, 1 + pieces)),
            dma(()),
            dma((2,)),
        ],
        compiler_params=pltpu.CompilerParams(
            collective_id=0, has_side_effects=True, vmem_limit_bytes=40 * 1024 * 1024
        ),
    )(*[pltpu.with_memory_space_constraint(a, pltpu.HBM) for a in (order, keys, values, gain, queries, residual, weight)])


def solution(mesh):
    in_specs = (
        P(("rep", "seq"), "head"),
        P(("rep", "seq"), "head"),
        P(("rep", "seq"), "head"),
        P(("rep", "seq"), "head"),
        P("head", None),
        P("head"),
        P("rep"),
    )
    out_specs = P(("rep", "seq"), "head")
    ns, nh = mesh.shape["seq"], mesh.shape["head"]
    return jax.shard_map(
        functools.partial(body, ns, nh),
        mesh=mesh,
        in_specs=in_specs,
        out_specs=out_specs,
        check_vma=False,
    )
```
